256 devices in a mesh: row: 16 (over x, y_hi, core), col: 16 (over y_lo, z).
Axes of the slice: x: 4, y: 4 (y_hi: 2, y_lo: 2; y = y_hi * 2 + y_lo), z: 8, core: 2. Of those that a mesh axis runs over, the one named last changes fastest.
Arguments:
- field: float32 [1, 256, 256, 512], P(None, 'row', 'col'), may hold values from -6 to 6
- shell: int32 [256, 256, 256], P(('row', 'col')), may hold values from 0 to 255
Outputs:
- power_modes: float32 [1, 256, 256, 256], P(None, ('row', 'col'))
- spectrum: float32 [1, 256], replicated
The draws below stay inside these ranges and needn't reach their ends.
All inputs are finite; a program needn't handle non-finite values.
Results may differ from the reference program's by a relative error of at most 0.0003.
Values sent between devices are 32-bit elements; how exact they have to be, the bound alone decides.
No kernel may reach another device: no remote copies, remote signals or barrier semaphores. Data moves between devices by JAX's collectives and lax.ppermute only.
A program may use at most 64 MiB of HBM per device.

```python
import math
import jax
import jax.numpy as jnp
import numpy as np
from jax import lax

NX = 256
NY = 256
NZ = 512
SHELLS = 256
FIELDS = 1
KZ = 256


def place_ends(entries, own_key, smallest, top_value):
    index_at = [jax.random.randint(jax.random.fold_in(own_key, axis), (), 0, length) for axis, length in enumerate(entries.shape)]
    longest = entries.shape.index(max(entries.shape))
    next_to = index_at[:longest] + [(index_at[longest] + 1) % entries.shape[longest]] + index_at[longest + 1:]
    return entries.at[tuple(index_at)].set(smallest).at[tuple(next_to)].set(top_value)


def steps_of(stream_key, extent, pieces, low, top_value):
    level, own = 1.0, jax.random.fold_in(stream_key, 6)
    for dim, parts in pieces:
        steps = jnp.exp(jax.random.uniform(jax.random.fold_in(own, dim), (parts,), jnp.float32, low / len(pieces), top_value / len(pieces)))
        level = level * jnp.repeat(steps, extent[dim] // parts).reshape([-1 if axis == dim else 1 for axis in range(len(extent))])
    return level


def rank_bounds(number_of, lean):
    loads = [(1 << 20) // math.isqrt(standing ** lean) + 1 for standing in range(1, number_of + 1)]
    spread = 1 + sum(loads) // (1 << 30)
    return np.cumsum(np.array([max(1, weight // spread) for weight in loads]))


def skewed_ids(stream_key, dims, amount, skew):
    listing = rank_bounds(amount, skew)
    pick = jax.random.randint(jax.random.fold_in(stream_key, 1), dims, 0, int(listing[amount - 1]))
    grade = jnp.searchsorted(jnp.asarray(listing, jnp.int32), pick, side="right")
    return jax.random.permutation(jax.random.fold_in(stream_key, 2), amount)[grade].astype(jnp.int32)


def scatter_about(rng, dims, width, limit, pieces=(), held_as=jnp.bfloat16):
    factor_of = steps_of(rng, dims, pieces, -0.22, 0.18) if pieces else 1.0
    drawn = jax.random.normal(rng, dims, jnp.float32) * width * factor_of
    return jnp.minimum(jnp.maximum(drawn, -limit), limit).astype(held_as)


def setup_inputs(seed: int = 0) -> dict:
    splits = jax.random.split(jax.random.key(seed), 3)
    field = scatter_about(splits[0], (FIELDS, NX, NY, NZ), 1.0, 6.0, ((1, 16), (2, 16)), jnp.float32)
    shell = place_ends(skewed_ids(splits[1], (KZ, NY, NX), SHELLS, 1), jax.random.fold_in(splits[1], 3), 0, SHELLS - 1).astype(jnp.int32)
    return dict(field=field, shell=shell)


def transform_one(single):
    spec = jnp.fft.rfftn(single)[:, :, :KZ]
    power = (jnp.real(spec) ** 2 + jnp.imag(spec) ** 2) / (NX * NY * NZ)
    return jnp.transpose(power, (2, 1, 0)).astype(jnp.float32)


def reference(field, shell):
    power_modes = lax.map(transform_one, field)
    labels = shell.reshape(-1).astype(jnp.int32)
    rows = []
    for index in range(FIELDS):
        sums = jax.ops.segment_sum(power_modes[index].reshape(-1), labels, num_segments=SHELLS)
        rows.append(sums)
    spectrum = (jnp.stack(rows) * (SHELLS / (KZ * NY * NX))).astype(jnp.float32)
    return power_modes, spectrum
```

```python
import functools
import math

import jax
import jax.numpy as jnp
import numpy as np
from jax import lax
from jax.experimental import pallas as pl
from jax.experimental.pallas import tpu as pltpu
from jax.sharding import Mesh
from jax.sharding import PartitionSpec as P

SHELLS = 256
ROW = ("row_0", "row_1", "row_2")
COL = ("col_0", "col_1")
ROW_COL = ROW + COL
F32 = jnp.float32
BF16 = jnp.bfloat16


def split_table(table):
    upper = table.astype(np.float32).astype(BF16)
    lower = (table - upper.astype(np.float64)).astype(np.float32).astype(BF16)
    return np.stack([upper, lower])


@functools.cache
def depth_tables(nz):
    half = nz // 2
    freqs = nz // 4
    z = np.arange(half)
    out = []
    for parity in range(2):
        k = 2 * np.arange(freqs) + parity
        angle = 2.0 * math.pi / nz * (k[:, None] * z[None, :] % nz)
        out.append(split_table(np.concatenate([np.cos(angle), -np.sin(angle)])))
    return np.stack(out)


@functools.cache
def plane_tables(radix):
    n = np.arange(radix)
    base = np.multiply.outer(n, n)
    both = base[:, None, :, None] + base[None, :, None, :]
    both = both.reshape(radix * radix, radix * radix)
    angle = 2.0 * math.pi / radix * (both % radix)
    square = np.stack([split_table(np.cos(angle)), split_table(-np.sin(angle))])
    angle = 2.0 * math.pi / (radix * radix) * (both % (radix * radix))
    twiddle = np.stack([np.cos(angle), -np.sin(angle)]).astype(np.float32)
    return square, twiddle


def split_two(values):
    upper = values.astype(BF16)
    return upper, (values - upper.astype(F32)).astype(BF16)


NN = (((1,), (0,)), ((), ()))
NT = (((1,), (1,)), ((), ()))


def dot3(lhs, rhs, dims):
    dot = functools.partial(lax.dot_general, dimension_numbers=dims, preferred_element_type=F32)
    return dot(lhs[0], rhs[0]) + dot(lhs[0], rhs[1]) + dot(lhs[1], rhs[0])


def depth_kernel(field_ref, table_ref, out_ref):
    half = field_ref.shape[1] // 2
    lanes = field_ref.shape[0] // 2
    freqs = table_ref.shape[2] // 2
    near = field_ref[:, :half]
    far = field_ref[:, half:]
    for parity in range(2):
        folded = split_two(near + far if parity == 0 else near - far)
        spec = dot3((table_ref[parity, 0], table_ref[parity, 1]), folded, NT)
        for part in range(2):
            for side in range(2):
                block = spec[part * freqs : (part + 1) * freqs, side * lanes : (side + 1) * lanes]
                out_ref[pl.ds(parity * 4 + part * 2 + side, freqs, stride=8), :] = block


def swap_digits(blocks, radix):
    lane = lax.broadcasted_iota(jnp.int32, blocks[0].shape, 1)
    width = blocks[0].shape[1]
    step = 1
    while step < radix:
        low = (lane & step) == 0
        out = list(blocks)
        for i in range(radix):
            if i & step:
                continue
            a, b = blocks[i], blocks[i + step]
            out[i] = jnp.where(low, a, pltpu.roll(b, step, 1))
            out[i + step] = jnp.where(low, pltpu.roll(a, width - step, 1), b)
        blocks = out
        step *= 2
    return blocks


def plane_kernel(scale, unit, recv_ref, square_ref, twiddle_ref, shell_ref, power_ref, sums_ref, acc_ref):
    n = power_ref.shape[0]
    radix = math.isqrt(n)
    parts = [
        jnp.concatenate([recv_ref[pl.ds(2 * c + s, n, stride=4), :] for s in range(2)], axis=1)
        for c in range(2)
    ]
    re, im = split_two(parts[0]), split_two(parts[1])
    cos = (square_ref[0, 0], square_ref[0, 1])
    sin = (square_ref[1, 0], square_ref[1, 1])
    u_re = dot3(cos, re, NN) - dot3(sin, im, NN)
    u_im = dot3(sin, re, NN) + dot3(cos, im, NN)
    t_re, t_im = twiddle_ref[0], twiddle_ref[1]
    re = split_two(u_re * t_re - u_im * t_im)
    im = split_two(u_re * t_im + u_im * t_re)
    v_re = dot3(re, cos, NN) - dot3(im, sin, NN)
    v_im = dot3(re, sin, NN) + dot3(im, cos, NN)
    power = (v_re * v_re + v_im * v_im) * scale
    half = n // 2
    for side in range(2):
        blocks = [
            power[a * radix : (a + 1) * radix, side * half : (side + 1) * half] for a in range(radix)
        ]
        for b, block in enumerate(swap_digits(blocks, radix)):
            power_ref[b * radix : (b + 1) * radix, side * half : (side + 1) * half] = block

    acc_ref[...] = jnp.zeros_like(acc_ref)

    def add_rows(index, carry):
        rows = pl.ds(index * 16, 16)
        upper, lower = split_two(power_ref[rows, :])
        marks = shell_ref[rows, :]
        high = (marks >> 4).astype(F32).astype(BF16)
        low = (marks & 15).astype(F32).astype(BF16)
        zero = jnp.zeros_like(upper)
        one = jnp.ones_like(upper)
        picks = [jnp.where(high == jnp.array(h, BF16), upper, zero) for h in range(16)]
        picks += [jnp.where(high == jnp.array(h, BF16), lower, zero) for h in range(16)]
        marked = [jnp.where(low == jnp.array(l, BF16), one, zero) for l in range(16)]
        acc_ref[...] += lax.dot_general(
            jnp.concatenate(picks, axis=0),
            jnp.concatenate(marked, axis=0),
            NT,
            preferred_element_type=F32,
        )
        return carry

    lax.fori_loop(0, n // 16, add_rows, 0)
    acc = acc_ref[:SHELLS, :] + acc_ref[SHELLS:, :]
    row = lax.broadcasted_iota(jnp.int32, (256, 256), 0)
    lane = lax.broadcasted_iota(jnp.int32, (256, 256), 1)
    same = jnp.where((row & 15) == (lane & 15), acc, 0.0)
    by_high = jnp.sum(same.reshape(16, 16, 256), axis=1)
    spread = ((row >> 4) == (lane & 15)).astype(F32).astype(BF16)
    upper = by_high.astype(BF16)
    rest = by_high - upper.astype(F32)
    middle, lower = split_two(rest)
    wide = sum(
        lax.dot_general(piece, spread, NN, preferred_element_type=F32)
        for piece in (upper, middle, lower)
    )
    row = lax.broadcasted_iota(jnp.int32, (16, 256), 0)
    lane = lax.broadcasted_iota(jnp.int32, (16, 256), 1)
    sums = jnp.sum(jnp.where((lane >> 4) == row, wide, 0.0), axis=0, keepdims=True) * unit
    for side in range(2):
        piece = sums[:, side * 128 : (side + 1) * 128]
        count = sums_ref.shape[0] // 2
        sums_ref[pl.ds(side, count, stride=2), :] = jnp.broadcast_to(piece, (count, 128))


def depth_call(field, tables):
    rows = field.shape[0]
    return pl.pallas_call(
        depth_kernel,
        out_shape=jax.ShapeDtypeStruct((field.shape[1] // 2 * 4, rows // 2), F32),
        name="depth",
    )(field, tables)


def plane_call(recv, square, twiddle, shell, devices, scale, unit):
    n = shell.shape[0]
    return pl.pallas_call(
        functools.partial(plane_kernel, scale, unit),
        out_shape=(
            jax.ShapeDtypeStruct((n, n), F32),
            jax.ShapeDtypeStruct((devices * 2, 128), F32),
        ),
        scratch_shapes=[pltpu.VMEM((2 * SHELLS, 256), F32)],
        name="plane",
    )(recv, square, twiddle, shell)


def local(field, shell):
    fields, cx, cy, nz = field.shape
    n_row = lax.axis_size(ROW)
    n_col = lax.axis_size(COL)
    devices = n_row * n_col
    nx, ny, keep = cx * n_row, cy * n_col, nz // 2
    square, twiddle = plane_tables(n_row)
    scale = 1.0 / (float(nx) * ny * nz)
    unit = float(SHELLS) / (keep * ny * nx)
    sent = depth_call(field.reshape(cx * cy, nz), depth_tables(nz))
    sent = sent.reshape(devices, 4, 128)
    got = lax.all_to_all(sent, ROW_COL, 0, 0, tiled=True)
    power, sums = plane_call(
        got.reshape(devices * 4, 128), square, twiddle, shell.reshape(ny, nx), devices, scale, unit
    )
    sums = lax.all_to_all(sums.reshape(devices, 2, 128), ROW_COL, 0, 0, tiled=True)
    spectrum = jnp.sum(sums, axis=0).reshape(fields, SHELLS)
    return (power.reshape(fields, 1, ny, nx), spectrum)


def solution(mesh):
    split = Mesh(mesh.devices.reshape(4, 2, 2, 2, 8), ROW_COL)
    in_specs = (P(None, ROW, COL, None), P(ROW_COL, None, None))
    out_specs = (P(None, ROW_COL, None, None), P())
    return jax.shard_map(local, mesh=split, in_specs=in_specs, out_specs=out_specs, check_vma=False)
```

```python
import functools
import math

import jax
import jax.numpy as jnp
import numpy as np
from jax import lax
from jax.experimental import pallas as pl
from jax.experimental.pallas import tpu as pltpu
from jax.sharding import Mesh
from jax.sharding import PartitionSpec as P

SHELLS = 256
ROW = ("row_0", "row_1", "row_2")
COL = ("col_0", "col_1")
ROW_COL = ROW + COL
F32 = jnp.float32
BF16 = jnp.bfloat16


def split_table(table):
    upper = table.astype(np.float32).astype(BF16)
    lower = (table - upper.astype(np.float64)).astype(np.float32).astype(BF16)
    return np.stack([upper, lower])


@functools.cache
def depth_tables(nz):
    half = nz // 2
    freqs = nz // 4
    z = np.arange(half)
    out = []
    for parity in range(2):
        k = 2 * np.arange(freqs) + parity
        angle = 2.0 * math.pi / nz * (k[:, None] * z[None, :] % nz)
        out.append(split_table(np.concatenate([np.cos(angle), -np.sin(angle)])))
    return np.stack(out)


@functools.cache
def plane_tables(radix):
    n = np.arange(radix)
    base = np.multiply.outer(n, n)
    both = base[:, None, :, None] + base[None, :, None, :]
    both = both.reshape(radix * radix, radix * radix)
    angle = 2.0 * math.pi / radix * (both % radix)
    square = np.stack([split_table(np.cos(angle)), split_table(-np.sin(angle))])
    angle = 2.0 * math.pi / (radix * radix) * (both % (radix * radix))
    twiddle = np.stack([np.cos(angle), -np.sin(angle)]).astype(np.float32)
    return square, twiddle


def split_two(values):
    upper = values.astype(BF16)
    return upper, (values - upper.astype(F32)).astype(BF16)


NN = (((1,), (0,)), ((), ()))
NT = (((1,), (1,)), ((), ()))


def dot3(lhs, rhs, dims):
    dot = functools.partial(lax.dot_general, dimension_numbers=dims, preferred_element_type=F32)
    return dot(lhs[0], rhs[0]) + dot(lhs[0], rhs[1]) + dot(lhs[1], rhs[0])


def depth_kernel(field_ref, table_ref, out_ref):
    half = field_ref.shape[1] // 2
    lanes = field_ref.shape[0] // 2
    freqs = table_ref.shape[2] // 2
    near = field_ref[:, :half]
    far = field_ref[:, half:]
    for parity in range(2):
        folded = split_two(near + far if parity == 0 else near - far)
        spec = dot3((table_ref[parity, 0], table_ref[parity, 1]), folded, NT)
        for part in range(2):
            for side in range(2):
                block = spec[part * freqs : (part + 1) * freqs, side * lanes : (side + 1) * lanes]
                out_ref[pl.ds(parity * 4 + part * 2 + side, freqs, stride=8), :] = block


def swap_digits(blocks, radix):
    lane = lax.broadcasted_iota(jnp.int32, blocks[0].shape, 1)
    width = blocks[0].shape[1]
    step = 1
    while step < radix:
        low = (lane & step) == 0
        out = list(blocks)
        for i in range(radix):
            if i & step:
                continue
            a, b = blocks[i], blocks[i + step]
            out[i] = jnp.where(low, a, pltpu.roll(b, step, 1))
            out[i + step] = jnp.where(low, pltpu.roll(a, width - step, 1), b)
        blocks = out
        step *= 2
    return blocks


def plane_kernel(scale, unit, recv_ref, square_ref, twiddle_ref, shell_ref, power_ref, sums_ref, acc_ref):
    n = power_ref.shape[0]
    radix = math.isqrt(n)
    parts = [
        jnp.concatenate([recv_ref[pl.ds(2 * c + s, n, stride=4), :] for s in range(2)], axis=1)
        for c in range(2)
    ]
    re, im = split_two(parts[0]), split_two(parts[1])
    cos = (square_ref[0, 0], square_ref[0, 1])
    sin = (square_ref[1, 0], square_ref[1, 1])
    u_re = dot3(cos, re, NN) - dot3(sin, im, NN)
    u_im = dot3(sin, re, NN) + dot3(cos, im, NN)
    t_re, t_im = twiddle_ref[0], twiddle_ref[1]
    re = split_two(u_re * t_re - u_im * t_im)
    im = split_two(u_re * t_im + u_im * t_re)
    v_re = dot3(re, cos, NN) - dot3(im, sin, NN)
    v_im = dot3(re, sin, NN) + dot3(im, cos, NN)
    power = (v_re * v_re + v_im * v_im) * scale
    half = n // 2
    for side in range(2):
        blocks = [
            power[a * radix : (a + 1) * radix, side * half : (side + 1) * half] for a in range(radix)
        ]
        for b, block in enumerate(swap_digits(blocks, radix)):
            power_ref[b * radix : (b + 1) * radix, side * half : (side + 1) * half] = block

    acc_ref[...] = jnp.zeros_like(acc_ref)

    def add_rows(index, carry):
        rows = pl.ds(index * 16, 16)
        upper, lower = split_two(power_ref[rows, :])
        marks = shell_ref[rows, :]
        high = (marks >> 4).astype(F32).astype(BF16)
        low = (marks & 15).astype(F32).astype(BF16)
        zero = jnp.zeros_like(upper)
        one = jnp.ones_like(upper)
        picks = [jnp.where(high == jnp.array(h, BF16), upper, zero) for h in range(16)]
        picks += [jnp.where(high == jnp.array(h, BF16), lower, zero) for h in range(16)]
        marked = [jnp.where(low == jnp.array(l, BF16), one, zero) for l in range(16)]
        acc_ref[...] += lax.dot_general(
            jnp.concatenate(picks, axis=0),
            jnp.concatenate(marked, axis=0),
            NT,
            preferred_element_type=F32,
        )
        return carry

    lax.fori_loop(0, n // 16, add_rows, 0)
    acc = acc_ref[:SHELLS, :] + acc_ref[SHELLS:, :]
    row = lax.broadcasted_iota(jnp.int32, (256, 256), 0)
    lane = lax.broadcasted_iota(jnp.int32, (256, 256), 1)
    same = jnp.where((row & 15) == (lane & 15), acc, 0.0)
    by_high = jnp.sum(same.reshape(16, 16, 256), axis=1)
    spread = ((row >> 4) == (lane & 15)).astype(F32).astype(BF16)
    upper = by_high.astype(BF16)
    rest = by_high - upper.astype(F32)
    middle, lower = split_two(rest)
    wide = sum(
        lax.dot_general(piece, spread, NN, preferred_element_type=F32)
        for piece in (upper, middle, lower)
    )
    row = lax.broadcasted_iota(jnp.int32, (16, 256), 0)
    lane = lax.broadcasted_iota(jnp.int32, (16, 256), 1)
    sums = jnp.sum(jnp.where((lane >> 4) == row, wide, 0.0), axis=0, keepdims=True) * unit
    for side in range(2):
        piece = sums[:, side * 128 : (side + 1) * 128]
        count = sums_ref.shape[0] // 2
        sums_ref[pl.ds(side, count, stride=2), :] = jnp.broadcast_to(piece, (count, 128))


def depth_call(field, tables):
    rows = field.shape[0]
    return pl.pallas_call(
        depth_kernel,
        out_shape=jax.ShapeDtypeStruct((field.shape[1] // 2 * 4, rows // 2), F32),
        compiler_params=pltpu.CompilerParams(vmem_limit_bytes=12 << 20),
        name="depth",
    )(field, tables)


def plane_call(recv, square, twiddle, shell, devices, scale, unit):
    n = shell.shape[0]
    return pl.pallas_call(
        functools.partial(plane_kernel, scale, unit),
        out_shape=(
            jax.ShapeDtypeStruct((n, n), F32),
            jax.ShapeDtypeStruct((devices * 2, 128), F32),
        ),
        scratch_shapes=[pltpu.VMEM((2 * SHELLS, 256), F32)],
        compiler_params=pltpu.CompilerParams(vmem_limit_bytes=16 << 20),
        name="plane",
    )(recv, square, twiddle, shell)


def local(field, shell):
    fields, cx, cy, nz = field.shape
    n_row = lax.axis_size(ROW)
    n_col = lax.axis_size(COL)
    devices = n_row * n_col
    nx, ny, keep = cx * n_row, cy * n_col, nz // 2
    square, twiddle = plane_tables(n_row)
    scale = 1.0 / (float(nx) * ny * nz)
    unit = float(SHELLS) / (keep * ny * nx)
    sent = depth_call(field.reshape(cx * cy, nz), depth_tables(nz))
    sent = sent.reshape(devices, 4, 128)
    got = lax.all_to_all(sent, ROW_COL, 0, 0, tiled=True)
    power, sums = plane_call(
        got.reshape(devices * 4, 128), square, twiddle, shell.reshape(ny, nx), devices, scale, unit
    )
    sums = lax.all_to_all(sums.reshape(devices, 2, 128), ROW_COL, 0, 0, tiled=True)
    spectrum = jnp.sum(sums, axis=0).reshape(fields, SHELLS)
    return (power.reshape(fields, 1, ny, nx), spectrum)


def solution(mesh):
    split = Mesh(mesh.devices.reshape(4, 2, 2, 2, 8), ROW_COL)
    in_specs = (P(None, ROW, COL, None), P(ROW_COL, None, None))
    out_specs = (P(None, ROW_COL, None, None), P())
    return jax.shard_map(local, mesh=split, in_specs=in_specs, out_specs=out_specs, check_vma=False)
```

```python
import functools
import math

import jax
import jax.numpy as jnp
import numpy as np
from jax import lax
from jax.experimental import pallas as pl
from jax.experimental.pallas import tpu as pltpu
from jax.sharding import Mesh
from jax.sharding import PartitionSpec as P

SHELLS = 256
ROW = ("row_0", "row_1", "row_2")
COL = ("col_0", "col_1")
ROW_COL = ROW + COL
CORE = "row_2"
CHIPS = ("row_0", "row_1", "col_0", "col_1")
F32 = jnp.float32
BF16 = jnp.bfloat16


def split_table(table):
    upper = table.astype(np.float32).astype(BF16)
    lower = (table - upper.astype(np.float64)).astype(np.float32).astype(BF16)
    return np.stack([upper, lower])


@functools.cache
def depth_tables(nz):
    half = nz // 2
    freqs = nz // 4
    z = np.arange(half)
    out = []
    for parity in range(2):
        k = 2 * np.arange(freqs) + parity
        angle = 2.0 * math.pi / nz * (k[:, None] * z[None, :] % nz)
        out.append(split_table(np.concatenate([np.cos(angle), -np.sin(angle)])))
    return np.stack(out)


@functools.cache
def plane_tables(radix):
    n = np.arange(radix)
    base = np.multiply.outer(n, n)
    both = base[:, None, :, None] + base[None, :, None, :]
    both = both.reshape(radix * radix, radix * radix)
    angle = 2.0 * math.pi / radix * (both % radix)
    square = np.stack([split_table(np.cos(angle)), split_table(-np.sin(angle))])
    angle = 2.0 * math.pi / (radix * radix) * (both % (radix * radix))
    twiddle = np.stack([np.cos(angle), -np.sin(angle)]).astype(np.float32)
    return square, twiddle


def split_two(values):
    upper = values.astype(BF16)
    return upper, (values - upper.astype(F32)).astype(BF16)


NN = (((1,), (0,)), ((), ()))
NT = (((1,), (1,)), ((), ()))


def dot3(lhs, rhs, dims):
    dot = functools.partial(lax.dot_general, dimension_numbers=dims, preferred_element_type=F32)
    return dot(lhs[0], rhs[0]) + dot(lhs[0], rhs[1]) + dot(lhs[1], rhs[0])


def depth_kernel(field_hbm, table_hbm, out_ref, field_ref, table_ref, sems):
    copies = [
        pltpu.make_async_copy(field_hbm, field_ref, sems.at[0]),
        pltpu.make_async_copy(table_hbm, table_ref, sems.at[1]),
    ]
    for copy in copies:
        copy.start()
    for copy in copies:
        copy.wait()
    half = field_ref.shape[1] // 2
    lanes = field_ref.shape[0] // 2
    freqs = table_ref.shape[2] // 2
    near = field_ref[:, :half]
    far = field_ref[:, half:]
    for parity in range(2):
        folded = split_two(near + far if parity == 0 else near - far)
        spec = dot3((table_ref[parity, 0], table_ref[parity, 1]), folded, NT)
        for part in range(2):
            for side in range(2):
                block = spec[part * freqs : (part + 1) * freqs, side * lanes : (side + 1) * lanes]
                out_ref[pl.ds(parity * 4 + part * 2 + side, freqs, stride=8), :] = block


def swap_digits(blocks, radix):
    lane = lax.broadcasted_iota(jnp.int32, blocks[0].shape, 1)
    width = blocks[0].shape[1]
    step = 1
    while step < radix:
        low = (lane & step) == 0
        out = list(blocks)
        for i in range(radix):
            if i & step:
                continue
            a, b = blocks[i], blocks[i + step]
            out[i] = jnp.where(low, a, pltpu.roll(b, step, 1))
            out[i + step] = jnp.where(low, pltpu.roll(a, width - step, 1), b)
        blocks = out
        step *= 2
    return blocks


def plane_kernel(
    scale, unit, recv_ref, square_ref, twiddle_ref, shell_ref, power_hbm, sums_ref, power_ref, sem
):
    n = power_ref.shape[0]
    radix = math.isqrt(n)
    parts = [
        jnp.concatenate([recv_ref[pl.ds(2 * c + s, n, stride=4), :] for s in range(2)], axis=1)
        for c in range(2)
    ]
    re, im = split_two(parts[0]), split_two(parts[1])
    cos = (square_ref[0, 0], square_ref[0, 1])
    sin = (square_ref[1, 0], square_ref[1, 1])
    u_re = dot3(cos, re, NN) - dot3(sin, im, NN)
    u_im = dot3(sin, re, NN) + dot3(cos, im, NN)
    t_re, t_im = twiddle_ref[0], twiddle_ref[1]
    re = split_two(u_re * t_re - u_im * t_im)
    im = split_two(u_re * t_im + u_im * t_re)
    v_re = dot3(re, cos, NN) - dot3(im, sin, NN)
    v_im = dot3(re, sin, NN) + dot3(im, cos, NN)
    power = (v_re * v_re + v_im * v_im) * scale
    half = n // 2
    for side in range(2):
        blocks = [
            power[a * radix : (a + 1) * radix, side * half : (side + 1) * half] for a in range(radix)
        ]
        for b, block in enumerate(swap_digits(blocks, radix)):
            power_ref[b * radix : (b + 1) * radix, side * half : (side + 1) * half] = block
    copy = pltpu.make_async_copy(power_ref, power_hbm, sem)
    copy.start()

    picks = []
    marked = []
    for index in range(n // 16):
        rows = slice(index * 16, (index + 1) * 16)
        upper, lower = split_two(power_ref[rows, :])
        marks = shell_ref[rows, :]
        high = (marks >> 4).astype(F32).astype(BF16)
        low = (marks & 15).astype(F32).astype(BF16)
        zero = jnp.zeros_like(upper)
        one = jnp.ones_like(upper)
        flags = [high == jnp.array(h, BF16) for h in range(16)]
        picks.append(
            jnp.concatenate(
                [jnp.where(flag, piece, zero) for piece in (upper, lower) for flag in flags], axis=0
            )
        )
        marked.append(
            jnp.concatenate(
                [jnp.where(low == jnp.array(l, BF16), one, zero) for l in range(16)], axis=0
            )
        )
    acc = lax.dot_general(
        jnp.concatenate(picks, axis=1),
        jnp.concatenate(marked, axis=1),
        NT,
        preferred_element_type=F32,
    )
    acc = acc[:SHELLS, :] + acc[SHELLS:, :]
    row = lax.broadcasted_iota(jnp.int32, (256, 256), 0)
    lane = lax.broadcasted_iota(jnp.int32, (256, 256), 1)
    same = jnp.where((row & 15) == (lane & 15), acc, 0.0)
    by_high = jnp.sum(same.reshape(16, 16, 256), axis=1)
    spread = ((row >> 4) == (lane & 15)).astype(F32).astype(BF16)
    upper = by_high.astype(BF16)
    rest = by_high - upper.astype(F32)
    middle, lower = split_two(rest)
    wide = sum(
        lax.dot_general(piece, spread, NN, preferred_element_type=F32)
        for piece in (upper, middle, lower)
    )
    row = lax.broadcasted_iota(jnp.int32, (16, 256), 0)
    lane = lax.broadcasted_iota(jnp.int32, (16, 256), 1)
    sums = jnp.sum(jnp.where((lane >> 4) == row, wide, 0.0), axis=0, keepdims=True) * unit
    for side in range(2):
        sums_ref[side : side + 1, :] = sums[:, side * 128 : (side + 1) * 128]
    copy.wait()


def depth_call(field, tables):
    rows = field.shape[0]
    return pl.pallas_call(
        depth_kernel,
        in_specs=[pl.BlockSpec(memory_space=pltpu.HBM)] * 2,
        out_shape=jax.ShapeDtypeStruct((field.shape[1] // 2 * 4, rows // 2), F32),
        scratch_shapes=[
            pltpu.VMEM(field.shape, field.dtype),
            pltpu.VMEM(tables.shape, tables.dtype),
            pltpu.SemaphoreType.DMA((2,)),
        ],
        compiler_params=pltpu.CompilerParams(vmem_limit_bytes=12 << 20),
        name="depth",
    )(field, tables)


def plane_call(recv, square, twiddle, shell, scale, unit):
    n = shell.shape[0]
    return pl.pallas_call(
        functools.partial(plane_kernel, scale, unit),
        out_shape=(
            jax.ShapeDtypeStruct((n, n), F32),
            jax.ShapeDtypeStruct((2, 128), F32),
        ),
        out_specs=(pl.BlockSpec(memory_space=pltpu.HBM), pl.BlockSpec(memory_space=pltpu.VMEM)),
        scratch_shapes=[pltpu.VMEM((n, n), F32), pltpu.SemaphoreType.DMA],
        compiler_params=pltpu.CompilerParams(vmem_limit_bytes=24 << 20),
        name="plane",
    )(recv, square, twiddle, shell)


def local(field, shell):
    fields, cx, cy, nz = field.shape
    n_row = lax.axis_size(ROW)
    n_col = lax.axis_size(COL)
    devices = n_row * n_col
    nx, ny, keep = cx * n_row, cy * n_col, nz // 2
    square, twiddle = plane_tables(n_row)
    scale = 1.0 / (float(nx) * ny * nz)
    unit = float(SHELLS) / (keep * ny * nx)
    sent = depth_call(field.reshape(cx * cy, nz), depth_tables(nz))
    sent = sent.reshape(devices, 4, 128)
    got = lax.all_to_all(sent, ROW_COL, 0, 0, tiled=True)
    power, sums = plane_call(
        got.reshape(devices * 4, 128), square, twiddle, shell.reshape(ny, nx), scale, unit
    )
    sums = sums + lax.ppermute(sums, CORE, [(0, 1), (1, 0)])
    chips = devices // lax.axis_size(CORE)
    sums = jnp.broadcast_to(sums, (chips, 2, 128))
    sums = lax.all_to_all(sums, CHIPS, 0, 0, tiled=True)
    spectrum = jnp.sum(sums, axis=0).reshape(fields, SHELLS)
    return (power.reshape(fields, 1, ny, nx), spectrum)


def solution(mesh):
    split = Mesh(mesh.devices.reshape(4, 2, 2, 2, 8), ROW_COL)
    in_specs = (P(None, ROW, COL, None), P(ROW_COL, None, None))
    out_specs = (P(None, ROW_COL, None, None), P())
    return jax.shard_map(local, mesh=split, in_specs=in_specs, out_specs=out_specs, check_vma=False)
```

```python
import functools
import math

import jax
import jax.numpy as jnp
import numpy as np
from jax import lax
from jax.experimental import pallas as pl
from jax.experimental.pallas import tpu as pltpu
from jax.sharding import Mesh
from jax.sharding import PartitionSpec as P

SHELLS = 256
ROW = ("row_0", "row_1", "row_2")
COL = ("col_0", "col_1")
ROW_COL = ROW + COL
CORE = "row_2"
CHIPS = ("row_0", "row_1", "col_0", "col_1")
F32 = jnp.float32
BF16 = jnp.bfloat16


def split_table(table):
    upper = table.astype(np.float32).astype(BF16)
    lower = (table - upper.astype(np.float64)).astype(np.float32).astype(BF16)
    return np.stack([upper, lower])


@functools.cache
def depth_tables(nz):
    half = nz // 2
    freqs = nz // 4
    z = np.arange(half)
    out = []
    for parity in range(2):
        k = 2 * np.arange(freqs) + parity
        angle = 2.0 * math.pi / nz * (k[:, None] * z[None, :] % nz)
        out.append(split_table(np.concatenate([np.cos(angle), -np.sin(angle)])))
    return np.stack(out)


@functools.cache
def plane_tables(radix):
    n = np.arange(radix)
    base = np.multiply.outer(n, n)
    both = base[:, None, :, None] + base[None, :, None, :]
    split = (radix, 2, radix // 2, radix * radix)
    size = (radix * radix, radix * radix)
    ordered = both.reshape(split).transpose(1, 0, 2, 3).reshape(size)
    both = both.reshape(size)
    unit = 2.0 * math.pi / radix
    left = np.stack([split_table(f(unit * (ordered % radix))) for f in (np.cos, minus_sin)])
    right = np.stack([split_table(f(unit * (both % radix))) for f in (np.cos, minus_sin)])
    angle = unit / radix * ordered
    twiddle = np.stack([np.cos(angle), -np.sin(angle)]).astype(np.float32)
    return left, right, twiddle


def minus_sin(angle):
    return -np.sin(angle)


def split_two(values):
    upper = values.astype(BF16)
    return upper, (values - upper.astype(F32)).astype(BF16)


NN = (((1,), (0,)), ((), ()))
NT = (((1,), (1,)), ((), ()))


def dot3(lhs, rhs, dims):
    dot = functools.partial(lax.dot_general, dimension_numbers=dims, preferred_element_type=F32)
    return dot(lhs[0], rhs[0]) + dot(lhs[0], rhs[1]) + dot(lhs[1], rhs[0])


def depth_kernel(field_hbm, table_hbm, out_ref, field_ref, table_ref, sems):
    copies = [
        pltpu.make_async_copy(field_hbm, field_ref, sems.at[0]),
        pltpu.make_async_copy(table_hbm, table_ref, sems.at[1]),
    ]
    for copy in copies:
        copy.start()
    for copy in copies:
        copy.wait()
    half = field_ref.shape[1] // 2
    lanes = field_ref.shape[0] // 2
    freqs = table_ref.shape[2] // 2
    near = field_ref[:, :half]
    far = field_ref[:, half:]
    for parity in range(2):
        folded = split_two(near + far if parity == 0 else near - far)
        spec = dot3((table_ref[parity, 0], table_ref[parity, 1]), folded, NT)
        for part in range(2):
            for side in range(2):
                block = spec[part * freqs : (part + 1) * freqs, side * lanes : (side + 1) * lanes]
                out_ref[pl.ds(parity * 4 + part * 2 + side, freqs, stride=8), :] = block


def swap_digits(blocks, radix):
    lane = lax.broadcasted_iota(jnp.int32, blocks[0].shape, 1)
    width = blocks[0].shape[1]
    step = 1
    while step < radix:
        low = (lane & step) == 0
        out = list(blocks)
        for i in range(radix):
            if i & step:
                continue
            a, b = blocks[i], blocks[i + step]
            out[i] = jnp.where(low, a, pltpu.roll(b, step, 1))
            out[i + step] = jnp.where(low, pltpu.roll(a, width - step, 1), b)
        blocks = out
        step *= 2
    return blocks


def plane_kernel(
    scale,
    unit,
    recv_ref,
    left_ref,
    right_ref,
    twiddle_ref,
    shell_ref,
    power_hbm,
    sums_ref,
    power_ref,
    sem,
):
    n = power_ref.shape[0]
    radix = math.isqrt(n)
    half = n // 2
    low_rows = radix // 2
    dot = functools.partial(lax.dot_general, preferred_element_type=F32)
    parts = [
        jnp.concatenate([recv_ref[pl.ds(2 * c + s, n, stride=4), :] for s in range(2)], axis=1)
        for c in range(2)
    ]
    re, im = split_two(parts[0]), split_two(parts[1])
    cos, sin = (left_ref[0, 0], left_ref[0, 1]), (left_ref[1, 0], left_ref[1, 1])
    to_re = jnp.concatenate([cos[0], -sin[0], cos[0], -sin[0], cos[1], -sin[1]], axis=1)
    to_im = jnp.concatenate([sin[0], cos[0], sin[0], cos[0], sin[1], cos[1]], axis=1)
    moved = jnp.concatenate([re[0], im[0], re[1], im[1], re[0], im[0]], axis=0)
    first = dot(jnp.concatenate([to_re, to_im], axis=0), moved, NN)
    cos, sin = (right_ref[0, 0], right_ref[0, 1]), (right_ref[1, 0], right_ref[1, 1])
    to_re = jnp.concatenate([cos[0], -sin[0], cos[0], -sin[0], cos[1], -sin[1]], axis=0)
    to_im = jnp.concatenate([sin[0], cos[0], sin[0], cos[0], sin[1], cos[1]], axis=0)

    picks = []
    marked = []
    for part in range(2):
        rows = slice(part * half, (part + 1) * half)
        u_re, u_im = first[rows, :], first[n + part * half : n + (part + 1) * half, :]
        t_re, t_im = twiddle_ref[0, rows, :], twiddle_ref[1, rows, :]
        re = split_two(u_re * t_re - u_im * t_im)
        im = split_two(u_re * t_im + u_im * t_re)
        turned = jnp.concatenate([re[0], im[0], re[1], im[1], re[0], im[0]], axis=1)
        v_re = dot(turned, to_re, NN)
        v_im = dot(turned, to_im, NN)
        power = (v_re * v_re + v_im * v_im) * scale
        sides = []
        for side in range(2):
            lanes = slice(side * half, (side + 1) * half)
            blocks = [power[a * low_rows : (a + 1) * low_rows, lanes] for a in range(radix)]
            sides.append(swap_digits(blocks, radix))
        tiles = [jnp.concatenate([sides[0][b], sides[1][b]], axis=1) for b in range(radix)]
        spots = [slice(b * radix + part * low_rows, b * radix + (part + 1) * low_rows) for b in range(radix)]
        for spot, tile in zip(spots, tiles):
            power_ref[spot, :] = tile
        for b in range(0, radix, 2):
            upper, lower = split_two(jnp.concatenate(tiles[b : b + 2], axis=0))
            marks = jnp.concatenate([shell_ref[spot, :] for spot in spots[b : b + 2]], axis=0)
            high = (marks >> 4).astype(F32).astype(BF16)
            low = (marks & 15).astype(F32).astype(BF16)
            zero = jnp.zeros_like(upper)
            one = jnp.ones_like(upper)
            flags = [high == jnp.array(h, BF16) for h in range(16)]
            picked = [jnp.where(flag, piece, zero) for piece in (upper, lower) for flag in flags]
            picks.append(jnp.concatenate(picked, axis=0))
            flags = [low == jnp.array(l, BF16) for l in range(16)]
            marked.append(jnp.concatenate([jnp.where(flag, one, zero) for flag in flags], axis=0))
    copy = pltpu.make_async_copy(power_ref, power_hbm, sem)
    copy.start()
    acc = dot(jnp.concatenate(picks, axis=1), jnp.concatenate(marked, axis=1), NT)
    acc = acc[:SHELLS, :] + acc[SHELLS:, :]
    row = lax.broadcasted_iota(jnp.int32, (256, 256), 0)
    lane = lax.broadcasted_iota(jnp.int32, (256, 256), 1)
    same = jnp.where((row & 15) == (lane & 15), acc, 0.0).reshape(16, 16, 256)
    by_high = (same[:, :8, :] + same[:, 8:, :]).reshape(128, 256)
    spread = ((row >> 4) == (lane & 15)).astype(F32).astype(BF16)
    upper, lower = split_two(by_high)
    wide = dot(upper, spread, NN) + dot(lower, spread, NN)
    row = lax.broadcasted_iota(jnp.int32, (128, 256), 0)
    lane = lax.broadcasted_iota(jnp.int32, (128, 256), 1)
    sums = jnp.sum(jnp.where((lane >> 4) == (row >> 3), wide, 0.0), axis=0, keepdims=True) * unit
    for side in range(2):
        sums_ref[side : side + 1, :] = sums[:, side * 128 : (side + 1) * 128]
    copy.wait()


def depth_call(field, tables):
    rows = field.shape[0]
    field = pltpu.with_memory_space_constraint(field, pltpu.HBM)
    tables = pltpu.with_memory_space_constraint(tables, pltpu.HBM)
    return pl.pallas_call(
        depth_kernel,
        in_specs=[pl.BlockSpec(memory_space=pltpu.HBM)] * 2,
        out_shape=jax.ShapeDtypeStruct((field.shape[1] // 2 * 4, rows // 2), F32),
        scratch_shapes=[
            pltpu.VMEM(field.shape, field.dtype),
            pltpu.VMEM(tables.shape, tables.dtype),
            pltpu.SemaphoreType.DMA((2,)),
        ],
        compiler_params=pltpu.CompilerParams(vmem_limit_bytes=12 << 20),
        name="depth",
    )(field, tables)


def plane_call(recv, left, right, twiddle, shell, scale, unit):
    n = shell.shape[0]
    return pl.pallas_call(
        functools.partial(plane_kernel, scale, unit),
        out_shape=(
            jax.ShapeDtypeStruct((n, n), F32),
            jax.ShapeDtypeStruct((2, 128), F32),
        ),
        out_specs=(pl.BlockSpec(memory_space=pltpu.HBM), pl.BlockSpec(memory_space=pltpu.VMEM)),
        scratch_shapes=[pltpu.VMEM((n, n), F32), pltpu.SemaphoreType.DMA],
        compiler_params=pltpu.CompilerParams(vmem_limit_bytes=24 << 20),
        name="plane",
    )(recv, left, right, twiddle, shell)


def local(field, shell):
    fields, cx, cy, nz = field.shape
    n_row = lax.axis_size(ROW)
    n_col = lax.axis_size(COL)
    devices = n_row * n_col
    nx, ny, keep = cx * n_row, cy * n_col, nz // 2
    left, right, twiddle = plane_tables(n_row)
    scale = 1.0 / (float(nx) * ny * nz)
    unit = float(SHELLS) / (keep * ny * nx)
    sent = depth_call(field.reshape(cx * cy, nz), jnp.asarray(depth_tables(nz)))
    sent = sent.reshape(devices, 4, 128)
    got = lax.all_to_all(sent, ROW_COL, 0, 0, tiled=True)
    got = got.reshape(devices * 4, 128)
    power, sums = plane_call(got, left, right, twiddle, shell.reshape(ny, nx), scale, unit)
    sums = sums + lax.ppermute(sums, CORE, [(0, 1), (1, 0)])
    chips = devices // lax.axis_size(CORE)
    sums = jnp.broadcast_to(sums, (chips, 2, 128))
    sums = lax.all_to_all(sums, CHIPS, 0, 0, tiled=True)
    spectrum = jnp.sum(sums, axis=0).reshape(fields, SHELLS)
    return (power.reshape(fields, 1, ny, nx), spectrum)


def solution(mesh):
    split = Mesh(mesh.devices.reshape(4, 2, 2, 2, 8), ROW_COL)
    in_specs = (P(None, ROW, COL, None), P(ROW_COL, None, None))
    out_specs = (P(None, ROW_COL, None, None), P())
    return jax.shard_map(local, mesh=split, in_specs=in_specs, out_specs=out_specs, check_vma=False)
```

```python
import functools
import math

import jax
import jax.numpy as jnp
import numpy as np
from jax import lax
from jax.experimental import pallas as pl
from jax.experimental.pallas import tpu as pltpu
from jax.sharding import Mesh
from jax.sharding import PartitionSpec as P

SHELLS = 256
ROW = ("row_0", "row_1", "row_2")
COL = ("col_0", "col_1")
ROW_COL = ROW + COL
CORE = "row_2"
CHIPS = ("row_0", "row_1", "col_0", "col_1")
F32 = jnp.float32
BF16 = jnp.bfloat16


def split_table(table):
    upper = table.astype(np.float32).astype(BF16)
    lower = (table - upper.astype(np.float64)).astype(np.float32).astype(BF16)
    return np.stack([upper, lower])


@functools.cache
def depth_tables(nz):
    half = nz // 2
    freqs = nz // 4
    z = np.arange(half)
    out = []
    for parity in range(2):
        k = 2 * np.arange(freqs) + parity
        angle = 2.0 * math.pi / nz * (k[:, None] * z[None, :] % nz)
        out.append(split_table(np.concatenate([np.cos(angle), -np.sin(angle)])))
    return np.stack(out)


@functools.cache
def plane_tables(radix):
    n = np.arange(radix)
    base = np.multiply.outer(n, n)
    both = base[:, None, :, None] + base[None, :, None, :]
    both = both.reshape(radix * radix, radix * radix)
    angle = 2.0 * math.pi / radix * (both % radix)
    square = np.stack([split_table(np.cos(angle)), split_table(-np.sin(angle))])
    angle = 2.0 * math.pi / (radix * radix) * (both % (radix * radix))
    twiddle = np.stack([np.cos(angle), -np.sin(angle)]).astype(np.float32)
    return square, twiddle


def split_two(values):
    upper = values.astype(BF16)
    return upper, (values - upper.astype(F32)).astype(BF16)


NN = (((1,), (0,)), ((), ()))
NT = (((1,), (1,)), ((), ()))


def dot3(lhs, rhs, dims):
    dot = functools.partial(lax.dot_general, dimension_numbers=dims, preferred_element_type=F32)
    return dot(lhs[0], rhs[0]) + dot(lhs[0], rhs[1]) + dot(lhs[1], rhs[0])


def depth_kernel(field_hbm, table_hbm, out_ref, field_ref, table_ref, sems):
    copies = [
        pltpu.make_async_copy(field_hbm, field_ref, sems.at[0]),
        pltpu.make_async_copy(table_hbm, table_ref, sems.at[1]),
    ]
    for copy in copies:
        copy.start()
    for copy in copies:
        copy.wait()
    half = field_ref.shape[1] // 2
    lanes = field_ref.shape[0] // 2
    freqs = table_ref.shape[2] // 2
    near = field_ref[:, :half]
    far = field_ref[:, half:]
    for parity in range(2):
        folded = split_two(near + far if parity == 0 else near - far)
        spec = dot3((table_ref[parity, 0], table_ref[parity, 1]), folded, NT)
        for part in range(2):
            for side in range(2):
                block = spec[part * freqs : (part + 1) * freqs, side * lanes : (side + 1) * lanes]
                out_ref[pl.ds(parity * 4 + part * 2 + side, freqs, stride=8), :] = block


def swap_digits(blocks, radix):
    lane = lax.broadcasted_iota(jnp.int32, blocks[0].shape, 1)
    width = blocks[0].shape[1]
    step = 1
    while step < radix:
        low = (lane & step) == 0
        out = list(blocks)
        for i in range(radix):
            if i & step:
                continue
            a, b = blocks[i], blocks[i + step]
            out[i] = jnp.where(low, a, pltpu.roll(b, step, 1))
            out[i + step] = jnp.where(low, pltpu.roll(a, width - step, 1), b)
        blocks = out
        step *= 2
    return blocks


def plane_kernel(
    scale, unit, recv_ref, square_ref, twiddle_ref, shell_ref, power_hbm, sums_ref, power_ref, sem
):
    n = power_ref.shape[0]
    radix = math.isqrt(n)
    parts = [
        jnp.concatenate([recv_ref[pl.ds(2 * c + s, n, stride=4), :] for s in range(2)], axis=1)
        for c in range(2)
    ]
    re, im = split_two(parts[0]), split_two(parts[1])
    cos = (square_ref[0, 0], square_ref[0, 1])
    sin = (square_ref[1, 0], square_ref[1, 1])
    u_re = dot3(cos, re, NN) - dot3(sin, im, NN)
    u_im = dot3(sin, re, NN) + dot3(cos, im, NN)
    t_re, t_im = twiddle_ref[0], twiddle_ref[1]
    re = split_two(u_re * t_re - u_im * t_im)
    im = split_two(u_re * t_im + u_im * t_re)
    v_re = dot3(re, cos, NN) - dot3(im, sin, NN)
    v_im = dot3(re, sin, NN) + dot3(im, cos, NN)
    power = (v_re * v_re + v_im * v_im) * scale
    half = n // 2
    picks = []
    marked = []
    for side in range(2):
        lanes = slice(side * half, (side + 1) * half)
        blocks = [power[a * radix : (a + 1) * radix, lanes] for a in range(radix)]
        for index, tile in enumerate(swap_digits(blocks, radix)):
            rows = slice(index * radix, (index + 1) * radix)
            power_ref[rows, lanes] = tile
            upper, lower = split_two(tile)
            marks = shell_ref[rows, lanes]
            high = (marks >> 4).astype(F32).astype(BF16)
            low = (marks & 15).astype(F32).astype(BF16)
            zero = jnp.zeros_like(upper)
            one = jnp.ones_like(upper)
            flags = [high == jnp.array(h, BF16) for h in range(16)]
            picked = [jnp.where(flag, piece, zero) for piece in (upper, lower) for flag in flags]
            picks.append(jnp.concatenate(picked, axis=0))
            flags = [low == jnp.array(l, BF16) for l in range(16)]
            picked = [jnp.where(flag, one, zero) for flag in flags]
            marked.append(jnp.concatenate(picked, axis=0))
    copy = pltpu.make_async_copy(power_ref, power_hbm, sem)
    copy.start()
    dot = functools.partial(lax.dot_general, preferred_element_type=F32)
    acc = dot(jnp.concatenate(picks, axis=1), jnp.concatenate(marked, axis=1), NT)
    acc = acc[:SHELLS, :] + acc[SHELLS:, :]
    row = lax.broadcasted_iota(jnp.int32, (256, 256), 0)
    lane = lax.broadcasted_iota(jnp.int32, (256, 256), 1)
    same = jnp.where((row & 15) == (lane & 15), acc, 0.0).reshape(16, 16, 256)
    by_high = (same[:, :8, :] + same[:, 8:, :]).reshape(128, 256)
    spread = ((row >> 4) == (lane & 15)).astype(F32).astype(BF16)
    upper, lower = split_two(by_high)
    wide = dot(upper, spread, NN) + dot(lower, spread, NN)
    row = lax.broadcasted_iota(jnp.int32, (128, 256), 0)
    lane = lax.broadcasted_iota(jnp.int32, (128, 256), 1)
    sums = jnp.sum(jnp.where((lane >> 4) == (row >> 3), wide, 0.0), axis=0, keepdims=True) * unit
    for side in range(2):
        sums_ref[side : side + 1, :] = sums[:, side * 128 : (side + 1) * 128]
    copy.wait()


def depth_call(field, tables):
    rows = field.shape[0]
    field = pltpu.with_memory_space_constraint(field, pltpu.HBM)
    tables = pltpu.with_memory_space_constraint(tables, pltpu.HBM)
    return pl.pallas_call(
        depth_kernel,
        in_specs=[pl.BlockSpec(memory_space=pltpu.HBM)] * 2,
        out_shape=jax.ShapeDtypeStruct((field.shape[1] // 2 * 4, rows // 2), F32),
        scratch_shapes=[
            pltpu.VMEM(field.shape, field.dtype),
            pltpu.VMEM(tables.shape, tables.dtype),
            pltpu.SemaphoreType.DMA((2,)),
        ],
        compiler_params=pltpu.CompilerParams(vmem_limit_bytes=12 << 20),
        name="depth",
    )(field, tables)


def plane_call(recv, square, twiddle, shell, scale, unit):
    n = shell.shape[0]
    return pl.pallas_call(
        functools.partial(plane_kernel, scale, unit),
        out_shape=(
            jax.ShapeDtypeStruct((n, n), F32),
            jax.ShapeDtypeStruct((2, 128), F32),
        ),
        out_specs=(pl.BlockSpec(memory_space=pltpu.HBM), pl.BlockSpec(memory_space=pltpu.VMEM)),
        scratch_shapes=[pltpu.VMEM((n, n), F32), pltpu.SemaphoreType.DMA],
        compiler_params=pltpu.CompilerParams(vmem_limit_bytes=24 << 20),
        name="plane",
    )(recv, square, twiddle, shell)


def local(field, shell):
    fields, cx, cy, nz = field.shape
    n_row = lax.axis_size(ROW)
    n_col = lax.axis_size(COL)
    devices = n_row * n_col
    nx, ny, keep = cx * n_row, cy * n_col, nz // 2
    square, twiddle = plane_tables(n_row)
    scale = 1.0 / (float(nx) * ny * nz)
    unit = float(SHELLS) / (keep * ny * nx)
    sent = depth_call(field.reshape(cx * cy, nz), jnp.asarray(depth_tables(nz)))
    sent = sent.reshape(devices, 4, 128)
    got = lax.all_to_all(sent, ROW_COL, 0, 0, tiled=True)
    got = got.reshape(devices * 4, 128)
    power, sums = plane_call(got, square, twiddle, shell.reshape(ny, nx), scale, unit)
    sums = sums + lax.ppermute(sums, CORE, [(0, 1), (1, 0)])
    chips = devices // lax.axis_size(CORE)
    sums = jnp.broadcast_to(sums, (chips, 2, 128))
    sums = lax.all_to_all(sums, CHIPS, 0, 0, tiled=True)
    spectrum = jnp.sum(sums, axis=0).reshape(fields, SHELLS)
    return (power.reshape(fields, 1, ny, nx), spectrum)


def solution(mesh):
    split = Mesh(mesh.devices.reshape(4, 2, 2, 2, 8), ROW_COL)
    in_specs = (P(None, ROW, COL, None), P(ROW_COL, None, None))
    out_specs = (P(None, ROW_COL, None, None), P())
    return jax.shard_map(local, mesh=split, in_specs=in_specs, out_specs=out_specs, check_vma=False)
```

```python
import functools
import itertools
import math

import jax
import jax.numpy as jnp
import numpy as np
from jax import lax
from jax.experimental import pallas as pl
from jax.experimental.pallas import tpu as pltpu
from jax.sharding import Mesh
from jax.sharding import PartitionSpec as P

SHELLS = 256
ROW = ("row_0", "row_1", "row_2")
COL = ("col_0", "col_1")
ROW_COL = ROW + COL
CORE = "row_2"
PEERS = ("row_0", "col_0", "col_1", "row_1", "row_2")
CHIPS = ("col_1", "col_0", "row_0", "row_1")
F32 = jnp.float32
BF16 = jnp.bfloat16


def split_table(table):
    upper = table.astype(np.float32).astype(BF16)
    lower = (table - upper.astype(np.float64)).astype(np.float32).astype(BF16)
    return np.stack([upper, lower])


def peer_order(sizes):
    ranks = np.arange(math.prod(sizes)).reshape(sizes)
    return ranks.transpose([ROW_COL.index(axis) for axis in PEERS]).reshape(-1)


def odd_step(sizes):
    return math.prod(sizes[ROW_COL.index(axis)] for axis in PEERS[PEERS.index(COL[-1]) + 1 :])


@functools.cache
def depth_tables(nz, sizes):
    order = peer_order(sizes).reshape(-1, 2, odd_step(sizes))
    z = np.arange(nz // 2)
    out = []
    for parity in range(2):
        k = order[:, parity, :].T.reshape(-1)
        angle = 2.0 * math.pi / nz * (k[:, None] * z[None, :] % nz)
        out.append(split_table(np.concatenate([np.cos(angle), -np.sin(angle)])))
    return np.stack(out)


@functools.cache
def plane_tables(radix, sizes):
    n = np.arange(radix)
    base = np.multiply.outer(n, n)
    both = base[:, None, :, None] + base[None, :, None, :]
    both = both.reshape(radix * radix, radix * radix)
    angle = 2.0 * math.pi / radix * (both % radix)
    square = np.stack([split_table(np.cos(angle)), split_table(-np.sin(angle))])
    angle = 2.0 * math.pi / (radix * radix) * both
    twiddle = np.stack([np.cos(angle), -np.sin(angle)]).astype(np.float32)
    return np.ascontiguousarray(square[..., peer_order(sizes)]), square, twiddle


def split_two(values):
    upper = values.astype(BF16)
    return upper, (values - upper.astype(F32)).astype(BF16)


NN = (((1,), (0,)), ((), ()))
NT = (((1,), (1,)), ((), ()))


def dot3(lhs, rhs, dims):
    dot = functools.partial(lax.dot_general, dimension_numbers=dims, preferred_element_type=F32)
    return dot(lhs[0], rhs[0]) + dot(lhs[0], rhs[1]) + dot(lhs[1], rhs[0])


def depth_kernel(step, field_hbm, table_hbm, out_ref, field_ref, table_ref, sems):
    copies = [
        pltpu.make_async_copy(field_hbm, field_ref, sems.at[0]),
        pltpu.make_async_copy(table_hbm, table_ref, sems.at[1]),
    ]
    for copy in copies:
        copy.start()
    for copy in copies:
        copy.wait()
    half = field_ref.shape[1] // 2
    lanes = field_ref.shape[0] // 2
    freqs = table_ref.shape[2] // 2
    near = field_ref[:, :half]
    far = field_ref[:, half:]
    for parity in range(2):
        folded = split_two(near + far if parity == 0 else near - far)
        spec = dot3((table_ref[parity, 0], table_ref[parity, 1]), folded, NT)
        count = freqs // step
        for part, low, side in itertools.product(range(2), range(step), range(2)):
            start = part * freqs + low * count
            block = spec[start : start + count, side * lanes : (side + 1) * lanes]
            start = (parity * step + low) * 4 + part * 2 + side
            out_ref[pl.ds(start, count, stride=8 * step), :] = block


def swap_digits(blocks, radix):
    lane = lax.broadcasted_iota(jnp.int32, blocks[0].shape, 1)
    width = blocks[0].shape[1]
    step = 1
    while step < radix:
        low = (lane & step) == 0
        out = list(blocks)
        for i in range(radix):
            if i & step:
                continue
            a, b = blocks[i], blocks[i + step]
            out[i] = jnp.where(low, a, pltpu.roll(b, step, 1))
            out[i + step] = jnp.where(low, pltpu.roll(a, width - step, 1), b)
        blocks = out
        step *= 2
    return blocks


def plane_kernel(
    scale, unit, recv_ref, left_ref, right_ref, twiddle_ref, shell_ref, power_hbm, sums_ref, power_ref, sem
):
    n = power_ref.shape[0]
    radix = math.isqrt(n)
    parts = [
        jnp.concatenate([recv_ref[pl.ds(2 * c + s, n, stride=4), :] for s in range(2)], axis=1)
        for c in range(2)
    ]
    re, im = split_two(parts[0]), split_two(parts[1])
    cos = (left_ref[0, 0], left_ref[0, 1])
    sin = (left_ref[1, 0], left_ref[1, 1])
    u_re = dot3(cos, re, NN) - dot3(sin, im, NN)
    u_im = dot3(sin, re, NN) + dot3(cos, im, NN)
    t_re, t_im = twiddle_ref[0], twiddle_ref[1]
    re = split_two(u_re * t_re - u_im * t_im)
    im = split_two(u_re * t_im + u_im * t_re)
    cos = (right_ref[0, 0], right_ref[0, 1])
    sin = (right_ref[1, 0], right_ref[1, 1])
    v_re = dot3(re, cos, NN) - dot3(im, sin, NN)
    v_im = dot3(re, sin, NN) + dot3(im, cos, NN)
    power = (v_re * v_re + v_im * v_im) * scale
    half = n // 2
    picks = []
    marked = []
    for side in range(2):
        lanes = slice(side * half, (side + 1) * half)
        blocks = [power[a * radix : (a + 1) * radix, lanes] for a in range(radix)]
        for index, tile in enumerate(swap_digits(blocks, radix)):
            rows = slice(index * radix, (index + 1) * radix)
            power_ref[rows, lanes] = tile
            upper, lower = split_two(tile)
            marks = shell_ref[rows, lanes]
            high = (marks >> 4).astype(F32).astype(BF16)
            low = (marks & 15).astype(F32).astype(BF16)
            zero = jnp.zeros_like(upper)
            one = jnp.ones_like(upper)
            flags = [high == jnp.array(h, BF16) for h in range(16)]
            picked = [jnp.where(flag, piece, zero) for piece in (upper, lower) for flag in flags]
            picks.append(jnp.concatenate(picked, axis=0))
            flags = [low == jnp.array(l, BF16) for l in range(16)]
            picked = [jnp.where(flag, one, zero) for flag in flags]
            marked.append(jnp.concatenate(picked, axis=0))
    copy = pltpu.make_async_copy(power_ref, power_hbm, sem)
    copy.start()
    dot = functools.partial(lax.dot_general, preferred_element_type=F32)
    acc = dot(jnp.concatenate(picks, axis=1), jnp.concatenate(marked, axis=1), NT)
    acc = acc[:SHELLS, :] + acc[SHELLS:, :]
    row = lax.broadcasted_iota(jnp.int32, (256, 256), 0)
    lane = lax.broadcasted_iota(jnp.int32, (256, 256), 1)
    same = jnp.where((row & 15) == (lane & 15), acc, 0.0).reshape(16, 16, 256)
    by_high = (same[:, :8, :] + same[:, 8:, :]).reshape(128, 256)
    spread = ((row >> 4) == (lane & 15)).astype(F32).astype(BF16)
    upper, lower = split_two(by_high)
    wide = dot(upper, spread, NN) + dot(lower, spread, NN)
    row = lax.broadcasted_iota(jnp.int32, (128, 256), 0)
    lane = lax.broadcasted_iota(jnp.int32, (128, 256), 1)
    sums = jnp.sum(jnp.where((lane >> 4) == (row >> 3), wide, 0.0), axis=0, keepdims=True) * unit
    for side in range(2):
        sums_ref[side : side + 1, :] = sums[:, side * 128 : (side + 1) * 128]
    copy.wait()


def depth_call(field, tables, step):
    rows = field.shape[0]
    field = pltpu.with_memory_space_constraint(field, pltpu.HBM)
    tables = pltpu.with_memory_space_constraint(tables, pltpu.HBM)
    return pl.pallas_call(
        functools.partial(depth_kernel, step),
        in_specs=[pl.BlockSpec(memory_space=pltpu.HBM)] * 2,
        out_shape=jax.ShapeDtypeStruct((field.shape[1] // 2 * 4, rows // 2), F32),
        scratch_shapes=[
            pltpu.VMEM(field.shape, field.dtype),
            pltpu.VMEM(tables.shape, tables.dtype),
            pltpu.SemaphoreType.DMA((2,)),
        ],
        compiler_params=pltpu.CompilerParams(vmem_limit_bytes=12 << 20),
        name="depth",
    )(field, tables)


def plane_call(recv, left, right, twiddle, shell, scale, unit):
    n = shell.shape[0]
    return pl.pallas_call(
        functools.partial(plane_kernel, scale, unit),
        out_shape=(
            jax.ShapeDtypeStruct((n, n), F32),
            jax.ShapeDtypeStruct((2, 128), F32),
        ),
        out_specs=(pl.BlockSpec(memory_space=pltpu.HBM), pl.BlockSpec(memory_space=pltpu.VMEM)),
        scratch_shapes=[pltpu.VMEM((n, n), F32), pltpu.SemaphoreType.DMA],
        compiler_params=pltpu.CompilerParams(vmem_limit_bytes=24 << 20),
        name="plane",
    )(recv, left, right, twiddle, shell)


def local(field, shell):
    fields, cx, cy, nz = field.shape
    n_row = lax.axis_size(ROW)
    n_col = lax.axis_size(COL)
    devices = n_row * n_col
    nx, ny, keep = cx * n_row, cy * n_col, nz // 2
    sizes = tuple(lax.axis_size(axis) for axis in ROW_COL)
    left, right, twiddle = plane_tables(n_row, sizes)
    scale = 1.0 / (float(nx) * ny * nz)
    unit = float(SHELLS) / (keep * ny * nx)
    sent = depth_call(field.reshape(cx * cy, nz), jnp.asarray(depth_tables(nz, sizes)), odd_step(sizes))
    sent = sent.reshape(devices, 4, 128)
    got = lax.all_to_all(sent, PEERS, 0, 0, tiled=True)
    got = got.reshape(devices * 4, 128)
    power, sums = plane_call(got, left, right, twiddle, shell.reshape(ny, nx), scale, unit)
    sums = sums + lax.ppermute(sums, CORE, [(0, 1), (1, 0)])
    chips = devices // lax.axis_size(CORE)
    sums = jnp.broadcast_to(sums, (chips, 2, 128))
    sums = lax.all_to_all(sums, CHIPS, 0, 0, tiled=True)
    spectrum = jnp.sum(sums, axis=0).reshape(fields, SHELLS)
    return (power.reshape(fields, 1, ny, nx), spectrum)


def solution(mesh):
    split = Mesh(mesh.devices.reshape(4, 2, 2, 2, 8), ROW_COL)
    in_specs = (P(None, ROW, COL, None), P(ROW_COL, None, None))
    out_specs = (P(None, ROW_COL, None, None), P())
    return jax.shard_map(local, mesh=split, in_specs=in_specs, out_specs=out_specs, check_vma=False)
```

```python
import functools
import itertools
import math

import jax
import jax.numpy as jnp
import numpy as np
from jax import lax
from jax.experimental import pallas as pl
from jax.experimental.pallas import tpu as pltpu
from jax.sharding import Mesh
from jax.sharding import PartitionSpec as P

SHELLS = 256
ROW = ("row_0", "row_1", "row_2")
COL = ("col_0", "col_1")
ROW_COL = ROW + COL
CORE = "row_2"
PEERS = ("col_0", "row_1", "row_0", "col_1", "row_2")
CHIPS = ("col_1", "col_0", "row_0", "row_1")
F32 = jnp.float32
BF16 = jnp.bfloat16


def split_table(table):
    upper = table.astype(np.float32).astype(BF16)
    lower = (table - upper.astype(np.float64)).astype(np.float32).astype(BF16)
    return np.stack([upper, lower])


def peer_order(sizes):
    ranks = np.arange(math.prod(sizes)).reshape(sizes)
    return ranks.transpose([ROW_COL.index(axis) for axis in PEERS]).reshape(-1)


def odd_step(sizes):
    return math.prod(sizes[ROW_COL.index(axis)] for axis in PEERS[PEERS.index(COL[-1]) + 1 :])


@functools.cache
def depth_tables(nz, sizes):
    order = peer_order(sizes).reshape(-1, 2, odd_step(sizes))
    z = np.arange(nz // 2)
    out = []
    for parity in range(2):
        k = order[:, parity, :].T.reshape(-1)
        angle = 2.0 * math.pi / nz * (k[:, None] * z[None, :] % nz)
        out.append(split_table(np.concatenate([np.cos(angle), -np.sin(angle)])))
    return np.stack(out)


@functools.cache
def plane_tables(radix, sizes):
    n = np.arange(radix)
    base = np.multiply.outer(n, n)
    both = base[:, None, :, None] + base[None, :, None, :]
    both = both.reshape(radix * radix, radix * radix)
    angle = 2.0 * math.pi / radix * (both % radix)
    square = np.stack([split_table(np.cos(angle)), split_table(-np.sin(angle))])
    angle = 2.0 * math.pi / (radix * radix) * both
    twiddle = np.stack([np.cos(angle), -np.sin(angle)]).astype(np.float32)
    return np.ascontiguousarray(square[..., peer_order(sizes)]), square, twiddle


def split_two(values):
    upper = values.astype(BF16)
    return upper, (values - upper.astype(F32)).astype(BF16)


NN = (((1,), (0,)), ((), ()))
NT = (((1,), (1,)), ((), ()))


def dot3(lhs, rhs, dims):
    dot = functools.partial(lax.dot_general, dimension_numbers=dims, preferred_element_type=F32)
    return dot(lhs[0], rhs[0]) + dot(lhs[0], rhs[1]) + dot(lhs[1], rhs[0])


def depth_kernel(step, field_hbm, table_hbm, out_ref, field_ref, table_ref, sems):
    tables = [
        pltpu.make_async_copy(table_hbm.at[parity], table_ref.at[parity], sems.at[parity])
        for parity in range(2)
    ]
    whole = pltpu.make_async_copy(field_hbm, field_ref, sems.at[2])
    tables[0].start()
    whole.start()
    tables[1].start()
    whole.wait()
    half = field_ref.shape[1] // 2
    lanes = field_ref.shape[0] // 2
    freqs = table_ref.shape[2] // 2
    near = field_ref[:, :half]
    far = field_ref[:, half:]
    for parity in range(2):
        tables[parity].wait()
        folded = split_two(near + far if parity == 0 else near - far)
        spec = dot3((table_ref[parity, 0], table_ref[parity, 1]), folded, NT)
        count = freqs // step
        for part, low, side in itertools.product(range(2), range(step), range(2)):
            start = part * freqs + low * count
            block = spec[start : start + count, side * lanes : (side + 1) * lanes]
            start = (parity * step + low) * 4 + part * 2 + side
            out_ref[pl.ds(start, count, stride=8 * step), :] = block


def swap_digits(blocks, radix):
    lane = lax.broadcasted_iota(jnp.int32, blocks[0].shape, 1)
    width = blocks[0].shape[1]
    step = 1
    while step < radix:
        low = (lane & step) == 0
        out = list(blocks)
        for i in range(radix):
            if i & step:
                continue
            a, b = blocks[i], blocks[i + step]
            out[i] = jnp.where(low, a, pltpu.roll(b, step, 1))
            out[i + step] = jnp.where(low, pltpu.roll(a, width - step, 1), b)
        blocks = out
        step *= 2
    return blocks


def plane_kernel(
    scale, unit, recv_ref, left_ref, right_ref, twiddle_ref, shell_ref, power_hbm, sums_ref, power_ref, sem
):
    n = power_ref.shape[0]
    radix = math.isqrt(n)
    parts = [
        jnp.concatenate([recv_ref[pl.ds(2 * c + s, n, stride=4), :] for s in range(2)], axis=1)
        for c in range(2)
    ]
    re, im = split_two(parts[0]), split_two(parts[1])
    cos = (left_ref[0, 0], left_ref[0, 1])
    sin = (left_ref[1, 0], left_ref[1, 1])
    u_re = dot3(cos, re, NN) - dot3(sin, im, NN)
    u_im = dot3(sin, re, NN) + dot3(cos, im, NN)
    t_re, t_im = twiddle_ref[0], twiddle_ref[1]
    re = split_two(u_re * t_re - u_im * t_im)
    im = split_two(u_re * t_im + u_im * t_re)
    cos = (right_ref[0, 0], right_ref[0, 1])
    sin = (right_ref[1, 0], right_ref[1, 1])
    v_re = dot3(re, cos, NN) - dot3(im, sin, NN)
    v_im = dot3(re, sin, NN) + dot3(im, cos, NN)
    power = (v_re * v_re + v_im * v_im) * scale
    half = n // 2
    picks = []
    marked = []
    for side in range(2):
        lanes = slice(side * half, (side + 1) * half)
        blocks = [power[a * radix : (a + 1) * radix, lanes] for a in range(radix)]
        for index, tile in enumerate(swap_digits(blocks, radix)):
            rows = slice(index * radix, (index + 1) * radix)
            power_ref[rows, lanes] = tile
            upper, lower = split_two(tile)
            marks = shell_ref[rows, lanes]
            high = (marks >> 4).astype(F32).astype(BF16)
            low = (marks & 15).astype(F32).astype(BF16)
            zero = jnp.zeros_like(upper)
            one = jnp.ones_like(upper)
            flags = [high == jnp.array(h, BF16) for h in range(16)]
            picked = [jnp.where(flag, piece, zero) for piece in (upper, lower) for flag in flags]
            picks.append(jnp.concatenate(picked, axis=0))
            flags = [low == jnp.array(l, BF16) for l in range(16)]
            picked = [jnp.where(flag, one, zero) for flag in flags]
            marked.append(jnp.concatenate(picked, axis=0))
    copy = pltpu.make_async_copy(power_ref, power_hbm, sem)
    copy.start()
    dot = functools.partial(lax.dot_general, preferred_element_type=F32)
    acc = dot(jnp.concatenate(picks, axis=1), jnp.concatenate(marked, axis=1), NT)
    acc = acc[:SHELLS, :] + acc[SHELLS:, :]
    row = lax.broadcasted_iota(jnp.int32, (256, 256), 0)
    lane = lax.broadcasted_iota(jnp.int32, (256, 256), 1)
    same = jnp.where((row & 15) == (lane & 15), acc, 0.0).reshape(16, 16, 256)
    by_high = (same[:, :8, :] + same[:, 8:, :]).reshape(128, 256)
    spread = ((row >> 4) == (lane & 15)).astype(F32).astype(BF16)
    upper, lower = split_two(by_high)
    wide = dot(upper, spread, NN) + dot(lower, spread, NN)
    row = lax.broadcasted_iota(jnp.int32, (128, 256), 0)
    lane = lax.broadcasted_iota(jnp.int32, (128, 256), 1)
    sums = jnp.sum(jnp.where((lane >> 4) == (row >> 3), wide, 0.0), axis=0, keepdims=True) * unit
    for side in range(2):
        sums_ref[side : side + 1, :] = sums[:, side * 128 : (side + 1) * 128]
    copy.wait()


def depth_call(field, tables, step):
    rows = field.shape[0]
    field = pltpu.with_memory_space_constraint(field, pltpu.HBM)
    tables = pltpu.with_memory_space_constraint(tables, pltpu.HBM)
    return pl.pallas_call(
        functools.partial(depth_kernel, step),
        in_specs=[pl.BlockSpec(memory_space=pltpu.HBM)] * 2,
        out_shape=jax.ShapeDtypeStruct((field.shape[1] // 2 * 4, rows // 2), F32),
        scratch_shapes=[
            pltpu.VMEM(field.shape, field.dtype),
            pltpu.VMEM(tables.shape, tables.dtype),
            pltpu.SemaphoreType.DMA((3,)),
        ],
        compiler_params=pltpu.CompilerParams(vmem_limit_bytes=12 << 20),
        name="depth",
    )(field, tables)


def plane_call(recv, left, right, twiddle, shell, scale, unit):
    n = shell.shape[0]
    return pl.pallas_call(
        functools.partial(plane_kernel, scale, unit),
        out_shape=(
            jax.ShapeDtypeStruct((n, n), F32),
            jax.ShapeDtypeStruct((2, 128), F32),
        ),
        out_specs=(pl.BlockSpec(memory_space=pltpu.HBM), pl.BlockSpec(memory_space=pltpu.VMEM)),
        scratch_shapes=[pltpu.VMEM((n, n), F32), pltpu.SemaphoreType.DMA],
        compiler_params=pltpu.CompilerParams(vmem_limit_bytes=24 << 20),
        name="plane",
    )(recv, left, right, twiddle, shell)


def local(field, shell):
    fields, cx, cy, nz = field.shape
    n_row = lax.axis_size(ROW)
    n_col = lax.axis_size(COL)
    devices = n_row * n_col
    nx, ny, keep = cx * n_row, cy * n_col, nz // 2
    sizes = tuple(lax.axis_size(axis) for axis in ROW_COL)
    left, right, twiddle = plane_tables(n_row, sizes)
    scale = 1.0 / (float(nx) * ny * nz)
    unit = float(SHELLS) / (keep * ny * nx)
    sent = depth_call(field.reshape(cx * cy, nz), jnp.asarray(depth_tables(nz, sizes)), odd_step(sizes))
    sent = sent.reshape(devices, 4, 128)
    got = lax.all_to_all(sent, PEERS, 0, 0, tiled=True)
    got = got.reshape(devices * 4, 128)
    power, sums = plane_call(got, left, right, twiddle, shell.reshape(ny, nx), scale, unit)
    sums = sums + lax.ppermute(sums, CORE, [(0, 1), (1, 0)])
    chips = devices // lax.axis_size(CORE)
    sums = jnp.broadcast_to(sums, (chips, 2, 128))
    sums = lax.all_to_all(sums, CHIPS, 0, 0, tiled=True)
    spectrum = jnp.sum(sums, axis=0).reshape(fields, SHELLS)
    return (power.reshape(fields, 1, ny, nx), spectrum)


def solution(mesh):
    split = Mesh(mesh.devices.reshape(4, 2, 2, 2, 8), ROW_COL)
    in_specs = (P(None, ROW, COL, None), P(ROW_COL, None, None))
    out_specs = (P(None, ROW_COL, None, None), P())
    return jax.shard_map(local, mesh=split, in_specs=in_specs, out_specs=out_specs, check_vma=False)
```

```python
import functools
import itertools
import math

import jax
import jax.numpy as jnp
import numpy as np
from jax import lax
from jax.experimental import pallas as pl
from jax.experimental.pallas import tpu as pltpu
from jax.sharding import Mesh
from jax.sharding import PartitionSpec as P

SHELLS = 256
ROW = ("row_0", "row_1", "row_2")
COL = ("col_0", "col_1")
ROW_COL = ROW + COL
CORE = "row_2"
PEERS = ("row_0", "col_0", "col_1", "row_1", "row_2")
CHIPS = ("col_1", "col_0", "row_0", "row_1")
F32 = jnp.float32
BF16 = jnp.bfloat16


def split_table(table):
    upper = table.astype(np.float32).astype(BF16)
    lower = (table - upper.astype(np.float64)).astype(np.float32).astype(BF16)
    return np.stack([upper, lower])


def peer_order(sizes):
    ranks = np.arange(math.prod(sizes)).reshape(sizes)
    return ranks.transpose([ROW_COL.index(axis) for axis in PEERS]).reshape(-1)


def odd_step(sizes):
    return math.prod(sizes[ROW_COL.index(axis)] for axis in PEERS[PEERS.index(COL[-1]) + 1 :])


@functools.cache
def depth_tables(nz, sizes):
    order = peer_order(sizes).reshape(-1, 2, odd_step(sizes))
    z = np.arange(nz // 2)
    out = []
    for parity in range(2):
        k = order[:, parity, :].T.reshape(-1)
        angle = 2.0 * math.pi / nz * (k[:, None] * z[None, :] % nz)
        out.append(split_table(np.concatenate([np.cos(angle), -np.sin(angle)])))
    return np.stack(out)


@functools.cache
def plane_tables(radix, sizes):
    n = np.arange(radix)
    base = np.multiply.outer(n, n)
    both = base[:, None, :, None] + base[None, :, None, :]
    both = both.reshape(radix * radix, radix * radix)
    angle = 2.0 * math.pi / radix * (both % radix)
    square = np.stack([split_table(np.cos(angle)), split_table(-np.sin(angle))])
    angle = 2.0 * math.pi / (radix * radix) * both
    twiddle = np.stack([np.cos(angle), -np.sin(angle)]).astype(np.float32)
    return np.ascontiguousarray(square[..., peer_order(sizes)]), square, twiddle


def split_two(values):
    upper = values.astype(BF16)
    return upper, (values - upper.astype(F32)).astype(BF16)


NN = (((1,), (0,)), ((), ()))
NT = (((1,), (1,)), ((), ()))


def dot3(lhs, rhs, dims):
    dot = functools.partial(lax.dot_general, dimension_numbers=dims, preferred_element_type=F32)
    return dot(lhs[0], rhs[0]) + dot(lhs[0], rhs[1]) + dot(lhs[1], rhs[0])


def depth_kernel(step, field_hbm, table_hbm, out_ref, field_ref, table_ref, sems):
    copies = [
        pltpu.make_async_copy(field_hbm, field_ref, sems.at[0]),
        pltpu.make_async_copy(table_hbm, table_ref, sems.at[1]),
    ]
    for copy in copies:
        copy.start()
    for copy in copies:
        copy.wait()
    half = field_ref.shape[1] // 2
    lanes = field_ref.shape[0] // 2
    freqs = table_ref.shape[2] // 2
    near = field_ref[:, :half]
    far = field_ref[:, half:]
    for parity in range(2):
        folded = split_two(near + far if parity == 0 else near - far)
        spec = dot3((table_ref[parity, 0], table_ref[parity, 1]), folded, NT)
        count = freqs // step
        for part, low, side in itertools.product(range(2), range(step), range(2)):
            start = part * freqs + low * count
            block = spec[start : start + count, side * lanes : (side + 1) * lanes]
            start = (parity * step + low) * 4 + part * 2 + side
            out_ref[pl.ds(start, count, stride=8 * step), :] = block


def swap_digits(blocks, radix):
    lane = lax.broadcasted_iota(jnp.int32, blocks[0].shape, 1)
    width = blocks[0].shape[1]
    step = 1
    while step < radix:
        low = (lane & step) == 0
        out = list(blocks)
        for i in range(radix):
            if i & step:
                continue
            a, b = blocks[i], blocks[i + step]
            out[i] = jnp.where(low, a, pltpu.roll(b, step, 1))
            out[i + step] = jnp.where(low, pltpu.roll(a, width - step, 1), b)
        blocks = out
        step *= 2
    return blocks


def plane_kernel(
    scale, unit, recv_ref, left_ref, twiddle_ref, right_hbm, shell_hbm, power_hbm, sums_ref, power_ref, right_ref, shell_ref, sems
):
    more = [
        pltpu.make_async_copy(right_hbm, right_ref, sems.at[0]),
        pltpu.make_async_copy(shell_hbm, shell_ref, sems.at[1]),
    ]
    for copy in more:
        copy.start()
    n = power_ref.shape[0]
    radix = math.isqrt(n)
    parts = [
        jnp.concatenate([recv_ref[pl.ds(2 * c + s, n, stride=4), :] for s in range(2)], axis=1)
        for c in range(2)
    ]
    re, im = split_two(parts[0]), split_two(parts[1])
    cos = (left_ref[0, 0], left_ref[0, 1])
    sin = (left_ref[1, 0], left_ref[1, 1])
    u_re = dot3(cos, re, NN) - dot3(sin, im, NN)
    u_im = dot3(sin, re, NN) + dot3(cos, im, NN)
    t_re, t_im = twiddle_ref[0], twiddle_ref[1]
    re = split_two(u_re * t_re - u_im * t_im)
    im = split_two(u_re * t_im + u_im * t_re)
    more[0].wait()
    cos = (right_ref[0, 0], right_ref[0, 1])
    sin = (right_ref[1, 0], right_ref[1, 1])
    v_re = dot3(re, cos, NN) - dot3(im, sin, NN)
    v_im = dot3(re, sin, NN) + dot3(im, cos, NN)
    power = (v_re * v_re + v_im * v_im) * scale
    half = n // 2
    more[1].wait()
    picks = []
    marked = []
    for side in range(2):
        lanes = slice(side * half, (side + 1) * half)
        blocks = [power[a * radix : (a + 1) * radix, lanes] for a in range(radix)]
        for index, tile in enumerate(swap_digits(blocks, radix)):
            rows = slice(index * radix, (index + 1) * radix)
            power_ref[rows, lanes] = tile
            upper, lower = split_two(tile)
            marks = shell_ref[rows, lanes]
            high = (marks >> 4).astype(F32).astype(BF16)
            low = (marks & 15).astype(F32).astype(BF16)
            zero = jnp.zeros_like(upper)
            one = jnp.ones_like(upper)
            flags = [high == jnp.array(h, BF16) for h in range(16)]
            picked = [jnp.where(flag, piece, zero) for piece in (upper, lower) for flag in flags]
            picks.append(jnp.concatenate(picked, axis=0))
            flags = [low == jnp.array(l, BF16) for l in range(16)]
            picked = [jnp.where(flag, one, zero) for flag in flags]
            marked.append(jnp.concatenate(picked, axis=0))
    copy = pltpu.make_async_copy(power_ref, power_hbm, sems.at[2])
    copy.start()
    dot = functools.partial(lax.dot_general, preferred_element_type=F32)
    acc = dot(jnp.concatenate(picks, axis=1), jnp.concatenate(marked, axis=1), NT)
    acc = acc[:SHELLS, :] + acc[SHELLS:, :]
    row = lax.broadcasted_iota(jnp.int32, (256, 256), 0)
    lane = lax.broadcasted_iota(jnp.int32, (256, 256), 1)
    same = jnp.where((row & 15) == (lane & 15), acc, 0.0).reshape(16, 16, 256)
    by_high = (same[:, :8, :] + same[:, 8:, :]).reshape(128, 256)
    spread = ((row >> 4) == (lane & 15)).astype(F32).astype(BF16)
    upper, lower = split_two(by_high)
    wide = dot(upper, spread, NN) + dot(lower, spread, NN)
    row = lax.broadcasted_iota(jnp.int32, (128, 256), 0)
    lane = lax.broadcasted_iota(jnp.int32, (128, 256), 1)
    sums = jnp.sum(jnp.where((lane >> 4) == (row >> 3), wide, 0.0), axis=0, keepdims=True) * unit
    for side in range(2):
        sums_ref[side : side + 1, :] = sums[:, side * 128 : (side + 1) * 128]
    copy.wait()


def depth_call(field, tables, step):
    rows = field.shape[0]
    field = pltpu.with_memory_space_constraint(field, pltpu.HBM)
    tables = pltpu.with_memory_space_constraint(tables, pltpu.HBM)
    return pl.pallas_call(
        functools.partial(depth_kernel, step),
        in_specs=[pl.BlockSpec(memory_space=pltpu.HBM)] * 2,
        out_shape=jax.ShapeDtypeStruct((field.shape[1] // 2 * 4, rows // 2), F32),
        scratch_shapes=[
            pltpu.VMEM(field.shape, field.dtype),
            pltpu.VMEM(tables.shape, tables.dtype),
            pltpu.SemaphoreType.DMA((2,)),
        ],
        compiler_params=pltpu.CompilerParams(vmem_limit_bytes=12 << 20),
        name="depth",
    )(field, tables)


def plane_call(recv, left, right, twiddle, shell, scale, unit):
    n = shell.shape[0]
    right = pltpu.with_memory_space_constraint(jnp.asarray(right), pltpu.HBM)
    shell = pltpu.with_memory_space_constraint(shell, pltpu.HBM)
    return pl.pallas_call(
        functools.partial(plane_kernel, scale, unit),
        out_shape=(
            jax.ShapeDtypeStruct((n, n), F32),
            jax.ShapeDtypeStruct((2, 128), F32),
        ),
        in_specs=[pl.BlockSpec(memory_space=pltpu.VMEM)] * 3 + [pl.BlockSpec(memory_space=pltpu.HBM)] * 2,
        out_specs=(pl.BlockSpec(memory_space=pltpu.HBM), pl.BlockSpec(memory_space=pltpu.VMEM)),
        scratch_shapes=[
            pltpu.VMEM((n, n), F32),
            pltpu.VMEM(right.shape, right.dtype),
            pltpu.VMEM(shell.shape, shell.dtype),
            pltpu.SemaphoreType.DMA((3,)),
        ],
        compiler_params=pltpu.CompilerParams(vmem_limit_bytes=24 << 20),
        name="plane",
    )(recv, left, twiddle, right, shell)


def local(field, shell):
    fields, cx, cy, nz = field.shape
    n_row = lax.axis_size(ROW)
    n_col = lax.axis_size(COL)
    devices = n_row * n_col
    nx, ny, keep = cx * n_row, cy * n_col, nz // 2
    sizes = tuple(lax.axis_size(axis) for axis in ROW_COL)
    left, right, twiddle = plane_tables(n_row, sizes)
    scale = 1.0 / (float(nx) * ny * nz)
    unit = float(SHELLS) / (keep * ny * nx)
    sent = depth_call(field.reshape(cx * cy, nz), jnp.asarray(depth_tables(nz, sizes)), odd_step(sizes))
    sent = sent.reshape(devices, 4, 128)
    got = lax.all_to_all(sent, PEERS, 0, 0, tiled=True)
    got = got.reshape(devices * 4, 128)
    power, sums = plane_call(got, left, right, twiddle, shell.reshape(ny, nx), scale, unit)
    sums = sums + lax.ppermute(sums, CORE, [(0, 1), (1, 0)])
    chips = devices // lax.axis_size(CORE)
    sums = jnp.broadcast_to(sums, (chips, 2, 128))
    sums = lax.all_to_all(sums, CHIPS, 0, 0, tiled=True)
    spectrum = jnp.sum(sums, axis=0).reshape(fields, SHELLS)
    return (power.reshape(fields, 1, ny, nx), spectrum)


def solution(mesh):
    split = Mesh(mesh.devices.reshape(4, 2, 2, 2, 8), ROW_COL)
    in_specs = (P(None, ROW, COL, None), P(ROW_COL, None, None))
    out_specs = (P(None, ROW_COL, None, None), P())
    return jax.shard_map(local, mesh=split, in_specs=in_specs, out_specs=out_specs, check_vma=False)
```

```python
import functools
import itertools
import math

import jax
import jax.numpy as jnp
import numpy as np
from jax import lax
from jax.experimental import pallas as pl
from jax.experimental.pallas import tpu as pltpu
from jax.sharding import Mesh
from jax.sharding import PartitionSpec as P

SHELLS = 256
ROW = ("row_0", "row_1", "row_2")
COL = ("col_0", "col_1", "col_2")
ROW_COL = ROW + COL
CORE = "row_2"
PEERS = ("row_0", "col_0", "col_1", "row_1", "row_2", "col_2")
CHIPS = ("col_1", "col_2", "col_0", "row_0", "row_1")
F32 = jnp.float32
BF16 = jnp.bfloat16


def split_table(table):
    upper = table.astype(np.float32).astype(BF16)
    lower = (table - upper.astype(np.float64)).astype(np.float32).astype(BF16)
    return np.stack([upper, lower])


def peer_order(sizes):
    ranks = np.arange(math.prod(sizes)).reshape(sizes)
    return ranks.transpose([ROW_COL.index(axis) for axis in PEERS]).reshape(-1)


def odd_step(sizes):
    return math.prod(sizes[ROW_COL.index(axis)] for axis in PEERS[PEERS.index(COL[-1]) + 1 :])


@functools.cache
def depth_tables(nz, sizes):
    order = peer_order(sizes).reshape(-1, 2, odd_step(sizes))
    z = np.arange(nz // 2)
    out = []
    for parity in range(2):
        k = order[:, parity, :].T.reshape(-1)
        angle = 2.0 * math.pi / nz * (k[:, None] * z[None, :] % nz)
        out.append(split_table(np.concatenate([np.cos(angle), -np.sin(angle)])))
    return np.stack(out)


@functools.cache
def plane_tables(radix, sizes):
    n = np.arange(radix)
    base = np.multiply.outer(n, n)
    both = base[:, None, :, None] + base[None, :, None, :]
    both = both.reshape(radix * radix, radix * radix)
    angle = 2.0 * math.pi / radix * (both % radix)
    square = np.stack([split_table(np.cos(angle)), split_table(-np.sin(angle))])
    angle = 2.0 * math.pi / (radix * radix) * both
    twiddle = np.stack([np.cos(angle), -np.sin(angle)]).astype(np.float32)
    return np.ascontiguousarray(square[..., peer_order(sizes)]), square, twiddle


def split_two(values):
    upper = values.astype(BF16)
    return upper, (values - upper.astype(F32)).astype(BF16)


NN = (((1,), (0,)), ((), ()))
NT = (((1,), (1,)), ((), ()))


def dot3(lhs, rhs, dims):
    dot = functools.partial(lax.dot_general, dimension_numbers=dims, preferred_element_type=F32)
    return dot(lhs[0], rhs[0]) + dot(lhs[0], rhs[1]) + dot(lhs[1], rhs[0])


def depth_kernel(step, field_hbm, table_hbm, out_ref, field_ref, table_ref, sems):
    copies = [
        pltpu.make_async_copy(field_hbm, field_ref, sems.at[0]),
        pltpu.make_async_copy(table_hbm, table_ref, sems.at[1]),
    ]
    for copy in copies:
        copy.start()
    for copy in copies:
        copy.wait()
    half = field_ref.shape[1] // 2
    lanes = field_ref.shape[0] // 2
    freqs = table_ref.shape[2] // 2
    near = field_ref[:, :half]
    far = field_ref[:, half:]
    for parity in range(2):
        folded = split_two(near + far if parity == 0 else near - far)
        spec = dot3((table_ref[parity, 0], table_ref[parity, 1]), folded, NT)
        count = freqs // step
        for part, low, side in itertools.product(range(2), range(step), range(2)):
            start = part * freqs + low * count
            block = spec[start : start + count, side * lanes : (side + 1) * lanes]
            start = (parity * step + low) * 4 + part * 2 + side
            out_ref[pl.ds(start, count, stride=8 * step), :] = block


def swap_digits(blocks, radix):
    lane = lax.broadcasted_iota(jnp.int32, blocks[0].shape, 1)
    width = blocks[0].shape[1]
    step = 1
    while step < radix:
        low = (lane & step) == 0
        out = list(blocks)
        for i in range(radix):
            if i & step:
                continue
            a, b = blocks[i], blocks[i + step]
            out[i] = jnp.where(low, a, pltpu.roll(b, step, 1))
            out[i + step] = jnp.where(low, pltpu.roll(a, width - step, 1), b)
        blocks = out
        step *= 2
    return blocks


def plane_kernel(
    scale, unit, recv_ref, left_ref, right_ref, twiddle_ref, shell_ref, power_hbm, sums_ref, power_ref, sem
):
    n = power_ref.shape[0]
    radix = math.isqrt(n)
    parts = [
        jnp.concatenate([recv_ref[pl.ds(2 * c + s, n, stride=4), :] for s in range(2)], axis=1)
        for c in range(2)
    ]
    re, im = split_two(parts[0]), split_two(parts[1])
    cos = (left_ref[0, 0], left_ref[0, 1])
    sin = (left_ref[1, 0], left_ref[1, 1])
    u_re = dot3(cos, re, NN) - dot3(sin, im, NN)
    u_im = dot3(sin, re, NN) + dot3(cos, im, NN)
    t_re, t_im = twiddle_ref[0], twiddle_ref[1]
    re = split_two(u_re * t_re - u_im * t_im)
    im = split_two(u_re * t_im + u_im * t_re)
    cos = (right_ref[0, 0], right_ref[0, 1])
    sin = (right_ref[1, 0], right_ref[1, 1])
    v_re = dot3(re, cos, NN) - dot3(im, sin, NN)
    v_im = dot3(re, sin, NN) + dot3(im, cos, NN)
    power = (v_re * v_re + v_im * v_im) * scale
    half = n // 2
    picks = []
    marked = []
    for side in range(2):
        lanes = slice(side * half, (side + 1) * half)
        blocks = [power[a * radix : (a + 1) * radix, lanes] for a in range(radix)]
        for index, tile in enumerate(swap_digits(blocks, radix)):
            rows = slice(index * radix, (index + 1) * radix)
            power_ref[rows, lanes] = tile
            upper, lower = split_two(tile)
            marks = shell_ref[rows, lanes]
            high = (marks >> 4).astype(F32).astype(BF16)
            low = (marks & 15).astype(F32).astype(BF16)
            zero = jnp.zeros_like(upper)
            one = jnp.ones_like(upper)
            flags = [high == jnp.array(h, BF16) for h in range(16)]
            picked = [jnp.where(flag, piece, zero) for piece in (upper, lower) for flag in flags]
            picks.append(jnp.concatenate(picked, axis=0))
            flags = [low == jnp.array(l, BF16) for l in range(16)]
            picked = [jnp.where(flag, one, zero) for flag in flags]
            marked.append(jnp.concatenate(picked, axis=0))
    copy = pltpu.make_async_copy(power_ref, power_hbm, sem)
    copy.start()
    dot = functools.partial(lax.dot_general, preferred_element_type=F32)
    acc = dot(jnp.concatenate(picks, axis=1), jnp.concatenate(marked, axis=1), NT)
    acc = acc[:SHELLS, :] + acc[SHELLS:, :]
    row = lax.broadcasted_iota(jnp.int32, (256, 256), 0)
    lane = lax.broadcasted_iota(jnp.int32, (256, 256), 1)
    same = jnp.where((row & 15) == (lane & 15), acc, 0.0).reshape(16, 16, 256)
    by_high = (same[:, :8, :] + same[:, 8:, :]).reshape(128, 256)
    spread = ((row >> 4) == (lane & 15)).astype(F32).astype(BF16)
    upper, lower = split_two(by_high)
    wide = dot(upper, spread, NN) + dot(lower, spread, NN)
    row = lax.broadcasted_iota(jnp.int32, (128, 256), 0)
    lane = lax.broadcasted_iota(jnp.int32, (128, 256), 1)
    sums = jnp.sum(jnp.where((lane >> 4) == (row >> 3), wide, 0.0), axis=0, keepdims=True) * unit
    for side in range(2):
        sums_ref[side : side + 1, :] = sums[:, side * 128 : (side + 1) * 128]
    copy.wait()


def depth_call(field, tables, step):
    rows = field.shape[0]
    field = pltpu.with_memory_space_constraint(field, pltpu.HBM)
    tables = pltpu.with_memory_space_constraint(tables, pltpu.HBM)
    return pl.pallas_call(
        functools.partial(depth_kernel, step),
        in_specs=[pl.BlockSpec(memory_space=pltpu.HBM)] * 2,
        out_shape=jax.ShapeDtypeStruct((field.shape[1] // 2 * 4, rows // 2), F32),
        scratch_shapes=[
            pltpu.VMEM(field.shape, field.dtype),
            pltpu.VMEM(tables.shape, tables.dtype),
            pltpu.SemaphoreType.DMA((2,)),
        ],
        compiler_params=pltpu.CompilerParams(vmem_limit_bytes=12 << 20),
        name="depth",
    )(field, tables)


def plane_call(recv, left, right, twiddle, shell, scale, unit):
    n = shell.shape[0]
    return pl.pallas_call(
        functools.partial(plane_kernel, scale, unit),
        out_shape=(
            jax.ShapeDtypeStruct((n, n), F32),
            jax.ShapeDtypeStruct((2, 128), F32),
        ),
        out_specs=(pl.BlockSpec(memory_space=pltpu.HBM), pl.BlockSpec(memory_space=pltpu.VMEM)),
        scratch_shapes=[pltpu.VMEM((n, n), F32), pltpu.SemaphoreType.DMA],
        compiler_params=pltpu.CompilerParams(vmem_limit_bytes=24 << 20),
        name="plane",
    )(recv, left, right, twiddle, shell)


def local(field, shell):
    fields, cx, cy, nz = field.shape
    n_row = lax.axis_size(ROW)
    n_col = lax.axis_size(COL)
    devices = n_row * n_col
    nx, ny, keep = cx * n_row, cy * n_col, nz // 2
    sizes = tuple(lax.axis_size(axis) for axis in ROW_COL)
    left, right, twiddle = plane_tables(n_row, sizes)
    scale = 1.0 / (float(nx) * ny * nz)
    unit = float(SHELLS) / (keep * ny * nx)
    sent = depth_call(field.reshape(cx * cy, nz), jnp.asarray(depth_tables(nz, sizes)), odd_step(sizes))
    sent = sent.reshape(devices, 4, 128)
    got = lax.all_to_all(sent, PEERS, 0, 0, tiled=True)
    got = got.reshape(devices * 4, 128)
    power, sums = plane_call(got, left, right, twiddle, shell.reshape(ny, nx), scale, unit)
    sums = sums + lax.ppermute(sums, CORE, [(0, 1), (1, 0)])
    chips = devices // lax.axis_size(CORE)
    sums = jnp.broadcast_to(sums, (chips, 2, 128))
    sums = lax.all_to_all(sums, CHIPS, 0, 0, tiled=True)
    spectrum = jnp.sum(sums, axis=0).reshape(fields, SHELLS)
    return (power.reshape(fields, 1, ny, nx), spectrum)


def solution(mesh):
    split = Mesh(mesh.devices.reshape(4, 2, 2, 2, 4, 2), ROW_COL)
    in_specs = (P(None, ROW, COL, None), P(ROW_COL, None, None))
    out_specs = (P(None, ROW_COL, None, None), P())
    return jax.shard_map(local, mesh=split, in_specs=in_specs, out_specs=out_specs, check_vma=False)
```

```python
import functools
import itertools
import math

import jax
import jax.numpy as jnp
import numpy as np
from jax import lax
from jax.experimental import pallas as pl
from jax.experimental.pallas import tpu as pltpu
from jax.sharding import Mesh
from jax.sharding import PartitionSpec as P

SHELLS = 256
ROW = ("row_0", "row_1", "row_2")
COL = ("col_0", "col_1", "col_2")
ROW_COL = ROW + COL
CORE = "row_2"
PEERS = ("row_0", "col_0", "col_1", "row_1", "row_2", "col_2")
CHIPS = ("col_1", "col_2", "col_0", "row_0", "row_1")
F32 = jnp.float32
BF16 = jnp.bfloat16


def split_table(table):
    upper = table.astype(np.float32).astype(BF16)
    lower = (table - upper.astype(np.float64)).astype(np.float32).astype(BF16)
    return np.stack([upper, lower])


def peer_order(sizes):
    ranks = np.arange(math.prod(sizes)).reshape(sizes)
    return ranks.transpose([ROW_COL.index(axis) for axis in PEERS]).reshape(-1)


def odd_step(sizes):
    return math.prod(sizes[ROW_COL.index(axis)] for axis in PEERS[PEERS.index(COL[-1]) + 1 :])


@functools.cache
def depth_tables(nz, sizes):
    order = peer_order(sizes).reshape(-1, 2, odd_step(sizes))
    z = np.arange(nz // 2)
    out = []
    for parity in range(2):
        k = order[:, parity, :].T.reshape(-1)
        angle = 2.0 * math.pi / nz * (k[:, None] * z[None, :] % nz)
        out.append(split_table(np.concatenate([np.cos(angle), -np.sin(angle)])))
    return np.stack(out)


@functools.cache
def plane_tables(radix, sizes):
    n = np.arange(radix)
    base = np.multiply.outer(n, n)
    both = base[:, None, :, None] + base[None, :, None, :]
    both = both.reshape(radix * radix, radix * radix)
    angle = 2.0 * math.pi / radix * (both % radix)
    cos, sin = np.cos(angle), -np.sin(angle)
    square = np.stack([split_table(table) for table in (cos, sin - cos, cos + sin)])
    angle = 2.0 * math.pi / (radix * radix) * both
    twiddle = np.stack([np.cos(angle), -np.sin(angle)]).astype(np.float32)
    return np.ascontiguousarray(square[..., peer_order(sizes)]), square, twiddle


def split_two(values):
    upper = values.astype(BF16)
    return upper, (values - upper.astype(F32)).astype(BF16)


NN = (((1,), (0,)), ((), ()))
NT = (((1,), (1,)), ((), ()))


def dot3(lhs, rhs, dims):
    dot = functools.partial(lax.dot_general, dimension_numbers=dims, preferred_element_type=F32)
    return dot(lhs[0], rhs[0]) + dot(lhs[0], rhs[1]) + dot(lhs[1], rhs[0])


def depth_kernel(step, field_hbm, table_hbm, out_ref, field_ref, table_ref, sems):
    copies = [
        pltpu.make_async_copy(field_hbm, field_ref, sems.at[0]),
        pltpu.make_async_copy(table_hbm, table_ref, sems.at[1]),
    ]
    for copy in copies:
        copy.start()
    for copy in copies:
        copy.wait()
    half = field_ref.shape[1] // 2
    lanes = field_ref.shape[0] // 2
    freqs = table_ref.shape[2] // 2
    near = field_ref[:, :half]
    far = field_ref[:, half:]
    for parity in range(2):
        folded = split_two(near + far if parity == 0 else near - far)
        spec = dot3((table_ref[parity, 0], table_ref[parity, 1]), folded, NT)
        count = freqs // step
        for part, low, side in itertools.product(range(2), range(step), range(2)):
            start = part * freqs + low * count
            block = spec[start : start + count, side * lanes : (side + 1) * lanes]
            start = (parity * step + low) * 4 + part * 2 + side
            out_ref[pl.ds(start, count, stride=8 * step), :] = block


def swap_digits(blocks, radix):
    lane = lax.broadcasted_iota(jnp.int32, blocks[0].shape, 1)
    width = blocks[0].shape[1]
    step = 1
    while step < radix:
        low = (lane & step) == 0
        out = list(blocks)
        for i in range(radix):
            if i & step:
                continue
            a, b = blocks[i], blocks[i + step]
            out[i] = jnp.where(low, a, pltpu.roll(b, step, 1))
            out[i + step] = jnp.where(low, pltpu.roll(a, width - step, 1), b)
        blocks = out
        step *= 2
    return blocks


def plane_kernel(
    scale, unit, recv_ref, left_ref, right_ref, twiddle_ref, shell_ref, power_hbm, sums_ref, power_ref, sem
):
    n = power_ref.shape[0]
    radix = math.isqrt(n)
    parts = [
        jnp.concatenate([recv_ref[pl.ds(2 * c + s, n, stride=4), :] for s in range(2)], axis=1)
        for c in range(2)
    ]
    tables = [(left_ref[i, 0], left_ref[i, 1]) for i in range(3)]
    factors = [split_two(x) for x in (parts[0] + parts[1], parts[0], parts[1])]
    both, more, less = [dot3(t, x, NN) for t, x in zip(tables, factors)]
    u_re, u_im = both - less, both + more
    t_re, t_im = twiddle_ref[0], twiddle_ref[1]
    re = u_re * t_re - u_im * t_im
    im = u_re * t_im + u_im * t_re
    tables = [(right_ref[i, 0], right_ref[i, 1]) for i in range(3)]
    factors = [split_two(x) for x in (re + im, re, im)]
    both, more, less = [dot3(x, t, NN) for t, x in zip(tables, factors)]
    v_re, v_im = both - less, both + more
    power = (v_re * v_re + v_im * v_im) * scale
    half = n // 2
    picks = []
    marked = []
    for side in range(2):
        lanes = slice(side * half, (side + 1) * half)
        blocks = [power[a * radix : (a + 1) * radix, lanes] for a in range(radix)]
        for index, tile in enumerate(swap_digits(blocks, radix)):
            rows = slice(index * radix, (index + 1) * radix)
            power_ref[rows, lanes] = tile
            upper, lower = split_two(tile)
            marks = shell_ref[rows, lanes]
            high = (marks >> 4).astype(F32).astype(BF16)
            low = (marks & 15).astype(F32).astype(BF16)
            zero = jnp.zeros_like(upper)
            one = jnp.ones_like(upper)
            flags = [high == jnp.array(h, BF16) for h in range(16)]
            picked = [jnp.where(flag, piece, zero) for piece in (upper, lower) for flag in flags]
            picks.append(jnp.concatenate(picked, axis=0))
            flags = [low == jnp.array(l, BF16) for l in range(16)]
            picked = [jnp.where(flag, one, zero) for flag in flags]
            marked.append(jnp.concatenate(picked, axis=0))
    copy = pltpu.make_async_copy(power_ref, power_hbm, sem)
    copy.start()
    dot = functools.partial(lax.dot_general, preferred_element_type=F32)
    acc = dot(jnp.concatenate(picks, axis=1), jnp.concatenate(marked, axis=1), NT)
    acc = acc[:SHELLS, :] + acc[SHELLS:, :]
    row = lax.broadcasted_iota(jnp.int32, (256, 256), 0)
    lane = lax.broadcasted_iota(jnp.int32, (256, 256), 1)
    same = jnp.where((row & 15) == (lane & 15), acc, 0.0).reshape(16, 16, 256)
    by_high = (same[:, :8, :] + same[:, 8:, :]).reshape(128, 256)
    spread = ((row >> 4) == (lane & 15)).astype(F32).astype(BF16)
    upper, lower = split_two(by_high)
    wide = dot(upper, spread, NN) + dot(lower, spread, NN)
    row = lax.broadcasted_iota(jnp.int32, (128, 256), 0)
    lane = lax.broadcasted_iota(jnp.int32, (128, 256), 1)
    sums = jnp.sum(jnp.where((lane >> 4) == (row >> 3), wide, 0.0), axis=0, keepdims=True) * unit
    for side in range(2):
        sums_ref[side : side + 1, :] = sums[:, side * 128 : (side + 1) * 128]
    copy.wait()


def depth_call(field, tables, step):
    rows = field.shape[0]
    field = pltpu.with_memory_space_constraint(field, pltpu.HBM)
    tables = pltpu.with_memory_space_constraint(tables, pltpu.HBM)
    return pl.pallas_call(
        functools.partial(depth_kernel, step),
        in_specs=[pl.BlockSpec(memory_space=pltpu.HBM)] * 2,
        out_shape=jax.ShapeDtypeStruct((field.shape[1] // 2 * 4, rows // 2), F32),
        scratch_shapes=[
            pltpu.VMEM(field.shape, field.dtype),
            pltpu.VMEM(tables.shape, tables.dtype),
            pltpu.SemaphoreType.DMA((2,)),
        ],
        compiler_params=pltpu.CompilerParams(vmem_limit_bytes=12 << 20),
        name="depth",
    )(field, tables)


def plane_call(recv, left, right, twiddle, shell, scale, unit):
    n = shell.shape[0]
    return pl.pallas_call(
        functools.partial(plane_kernel, scale, unit),
        out_shape=(
            jax.ShapeDtypeStruct((n, n), F32),
            jax.ShapeDtypeStruct((2, 128), F32),
        ),
        out_specs=(pl.BlockSpec(memory_space=pltpu.HBM), pl.BlockSpec(memory_space=pltpu.VMEM)),
        scratch_shapes=[pltpu.VMEM((n, n), F32), pltpu.SemaphoreType.DMA],
        compiler_params=pltpu.CompilerParams(vmem_limit_bytes=24 << 20),
        name="plane",
    )(recv, left, right, twiddle, shell)


def local(field, shell):
    fields, cx, cy, nz = field.shape
    n_row = lax.axis_size(ROW)
    n_col = lax.axis_size(COL)
    devices = n_row * n_col
    nx, ny, keep = cx * n_row, cy * n_col, nz // 2
    sizes = tuple(lax.axis_size(axis) for axis in ROW_COL)
    left, right, twiddle = plane_tables(n_row, sizes)
    scale = 1.0 / (float(nx) * ny * nz)
    unit = float(SHELLS) / (keep * ny * nx)
    sent = depth_call(field.reshape(cx * cy, nz), jnp.asarray(depth_tables(nz, sizes)), odd_step(sizes))
    sent = sent.reshape(devices, 4, 128)
    got = lax.all_to_all(sent, PEERS, 0, 0, tiled=True)
    got = got.reshape(devices * 4, 128)
    power, sums = plane_call(got, left, right, twiddle, shell.reshape(ny, nx), scale, unit)
    sums = sums + lax.ppermute(sums, CORE, [(0, 1), (1, 0)])
    chips = devices // lax.axis_size(CORE)
    sums = jnp.broadcast_to(sums, (chips, 2, 128))
    sums = lax.all_to_all(sums, CHIPS, 0, 0, tiled=True)
    spectrum = jnp.sum(sums, axis=0).reshape(fields, SHELLS)
    return (power.reshape(fields, 1, ny, nx), spectrum)


def solution(mesh):
    split = Mesh(mesh.devices.reshape(4, 2, 2, 2, 4, 2), ROW_COL)
    in_specs = (P(None, ROW, COL, None), P(ROW_COL, None, None))
    out_specs = (P(None, ROW_COL, None, None), P())
    return jax.shard_map(local, mesh=split, in_specs=in_specs, out_specs=out_specs, check_vma=False)
```

```python
import functools
import itertools
import math

import jax
import jax.numpy as jnp
import numpy as np
from jax import lax
from jax.experimental import pallas as pl
from jax.experimental.pallas import tpu as pltpu
from jax.sharding import Mesh
from jax.sharding import PartitionSpec as P

SHELLS = 256
ROW = ("row_0", "row_1", "row_2")
COL = ("col_0", "col_1", "col_2")
ROW_COL = ROW + COL
CORE = "row_2"
PEERS = ("row_0", "col_0", "col_1", "row_1", "col_2", "row_2")
CHIPS = ("col_1", "col_2", "col_0", "row_0", "row_1")
F32 = jnp.float32
BF16 = jnp.bfloat16


def split_table(table):
    upper = table.astype(np.float32).astype(BF16)
    lower = (table - upper.astype(np.float64)).astype(np.float32).astype(BF16)
    return np.stack([upper, lower])


def peer_order(sizes):
    ranks = np.arange(math.prod(sizes)).reshape(sizes)
    return ranks.transpose([ROW_COL.index(axis) for axis in PEERS]).reshape(-1)


def odd_step(sizes):
    return math.prod(sizes[ROW_COL.index(axis)] for axis in PEERS[PEERS.index(COL[-1]) + 1 :])


@functools.cache
def depth_tables(nz, sizes):
    order = peer_order(sizes).reshape(-1, 2, odd_step(sizes))
    z = np.arange(nz // 2)
    out = []
    for parity in range(2):
        k = order[:, parity, :].T.reshape(-1)
        angle = 2.0 * math.pi / nz * (k[:, None] * z[None, :] % nz)
        out.append(split_table(np.concatenate([np.cos(angle), -np.sin(angle)])))
    return np.stack(out)


@functools.cache
def plane_tables(radix, sizes):
    n = np.arange(radix)
    base = np.multiply.outer(n, n)
    both = base[:, None, :, None] + base[None, :, None, :]
    both = both.reshape(radix * radix, radix * radix)
    angle = 2.0 * math.pi / radix * (both % radix)
    cos, sin = np.cos(angle), -np.sin(angle)
    square = np.stack([split_table(table) for table in (cos, sin - cos, cos + sin)])
    angle = 2.0 * math.pi / (radix * radix) * both
    twiddle = np.stack([np.cos(angle), -np.sin(angle)]).astype(np.float32)
    return np.ascontiguousarray(square[..., peer_order(sizes)]), square, twiddle


def split_two(values):
    upper = values.astype(BF16)
    return upper, (values - upper.astype(F32)).astype(BF16)


NN = (((1,), (0,)), ((), ()))
NT = (((1,), (1,)), ((), ()))


def dot3(lhs, rhs, dims):
    dot = functools.partial(lax.dot_general, dimension_numbers=dims, preferred_element_type=F32)
    return dot(lhs[0], rhs[0]) + dot(lhs[0], rhs[1]) + dot(lhs[1], rhs[0])


def depth_kernel(step, field_hbm, table_hbm, out_ref, field_ref, table_ref, sems):
    copies = [
        pltpu.make_async_copy(field_hbm, field_ref, sems.at[0]),
        pltpu.make_async_copy(table_hbm, table_ref, sems.at[1]),
    ]
    for copy in copies:
        copy.start()
    for copy in copies:
        copy.wait()
    half = field_ref.shape[1] // 2
    lanes = field_ref.shape[0] // 2
    freqs = table_ref.shape[2] // 2
    near = field_ref[:, :half]
    far = field_ref[:, half:]
    for parity in range(2):
        folded = split_two(near + far if parity == 0 else near - far)
        spec = dot3((table_ref[parity, 0], table_ref[parity, 1]), folded, NT)
        count = freqs // step
        for part, low, side in itertools.product(range(2), range(step), range(2)):
            start = part * freqs + low * count
            block = spec[start : start + count, side * lanes : (side + 1) * lanes]
            start = (parity * step + low) * 4 + part * 2 + side
            out_ref[pl.ds(start, count, stride=8 * step), :] = block


def swap_digits(blocks, radix):
    lane = lax.broadcasted_iota(jnp.int32, blocks[0].shape, 1)
    width = blocks[0].shape[1]
    step = 1
    while step < radix:
        low = (lane & step) == 0
        out = list(blocks)
        for i in range(radix):
            if i & step:
                continue
            a, b = blocks[i], blocks[i + step]
            out[i] = jnp.where(low, a, pltpu.roll(b, step, 1))
            out[i + step] = jnp.where(low, pltpu.roll(a, width - step, 1), b)
        blocks = out
        step *= 2
    return blocks


def plane_kernel(
    scale, unit, recv_ref, left_ref, right_ref, twiddle_ref, shell_ref, power_hbm, sums_ref, power_ref, sem
):
    n = power_ref.shape[0]
    radix = math.isqrt(n)
    parts = [
        jnp.concatenate([recv_ref[pl.ds(2 * c + s, n, stride=4), :] for s in range(2)], axis=1)
        for c in range(2)
    ]
    tables = [(left_ref[i, 0], left_ref[i, 1]) for i in range(3)]
    factors = [split_two(x) for x in (parts[0] + parts[1], parts[0], parts[1])]
    both, more, less = [dot3(t, x, NN) for t, x in zip(tables, factors)]
    u_re, u_im = both - less, both + more
    t_re, t_im = twiddle_ref[0], twiddle_ref[1]
    re = u_re * t_re - u_im * t_im
    im = u_re * t_im + u_im * t_re
    tables = [(right_ref[i, 0], right_ref[i, 1]) for i in range(3)]
    factors = [split_two(x) for x in (re + im, re, im)]
    both, more, less = [dot3(x, t, NN) for t, x in zip(tables, factors)]
    v_re, v_im = both - less, both + more
    power = (v_re * v_re + v_im * v_im) * scale
    half = n // 2
    picks = []
    marked = []
    for side in range(2):
        lanes = slice(side * half, (side + 1) * half)
        blocks = [power[a * radix : (a + 1) * radix, lanes] for a in range(radix)]
        for index, tile in enumerate(swap_digits(blocks, radix)):
            rows = slice(index * radix, (index + 1) * radix)
            power_ref[rows, lanes] = tile
            upper, lower = split_two(tile)
            marks = shell_ref[rows, lanes]
            high = (marks >> 4).astype(F32).astype(BF16)
            low = (marks & 15).astype(F32).astype(BF16)
            zero = jnp.zeros_like(upper)
            one = jnp.ones_like(upper)
            flags = [high == jnp.array(h, BF16) for h in range(16)]
            picked = [jnp.where(flag, piece, zero) for piece in (upper, lower) for flag in flags]
            picks.append(jnp.concatenate(picked, axis=0))
            flags = [low == jnp.array(l, BF16) for l in range(16)]
            picked = [jnp.where(flag, one, zero) for flag in flags]
            marked.append(jnp.concatenate(picked, axis=0))
    copy = pltpu.make_async_copy(power_ref, power_hbm, sem)
    copy.start()
    dot = functools.partial(lax.dot_general, preferred_element_type=F32)
    acc = dot(jnp.concatenate(picks, axis=1), jnp.concatenate(marked, axis=1), NT)
    acc = acc[:SHELLS, :] + acc[SHELLS:, :]
    row = lax.broadcasted_iota(jnp.int32, (256, 256), 0)
    lane = lax.broadcasted_iota(jnp.int32, (256, 256), 1)
    same = jnp.where((row & 15) == (lane & 15), acc, 0.0).reshape(16, 16, 256)
    by_high = (same[:, :8, :] + same[:, 8:, :]).reshape(128, 256)
    spread = ((row >> 4) == (lane & 15)).astype(F32).astype(BF16)
    upper, lower = split_two(by_high)
    wide = dot(upper, spread, NN) + dot(lower, spread, NN)
    row = lax.broadcasted_iota(jnp.int32, (128, 256), 0)
    lane = lax.broadcasted_iota(jnp.int32, (128, 256), 1)
    sums = jnp.sum(jnp.where((lane >> 4) == (row >> 3), wide, 0.0), axis=0, keepdims=True) * unit
    for side in range(2):
        sums_ref[side : side + 1, :] = sums[:, side * 128 : (side + 1) * 128]
    copy.wait()


def depth_call(field, tables, step):
    rows = field.shape[0]
    field = pltpu.with_memory_space_constraint(field, pltpu.HBM)
    tables = pltpu.with_memory_space_constraint(tables, pltpu.HBM)
    return pl.pallas_call(
        functools.partial(depth_kernel, step),
        in_specs=[pl.BlockSpec(memory_space=pltpu.HBM)] * 2,
        out_shape=jax.ShapeDtypeStruct((field.shape[1] // 2 * 4, rows // 2), F32),
        scratch_shapes=[
            pltpu.VMEM(field.shape, field.dtype),
            pltpu.VMEM(tables.shape, tables.dtype),
            pltpu.SemaphoreType.DMA((2,)),
        ],
        compiler_params=pltpu.CompilerParams(vmem_limit_bytes=12 << 20),
        name="depth",
    )(field, tables)


def plane_call(recv, left, right, twiddle, shell, scale, unit):
    n = shell.shape[0]
    return pl.pallas_call(
        functools.partial(plane_kernel, scale, unit),
        out_shape=(
            jax.ShapeDtypeStruct((n, n), F32),
            jax.ShapeDtypeStruct((2, 128), F32),
        ),
        out_specs=(pl.BlockSpec(memory_space=pltpu.HBM), pl.BlockSpec(memory_space=pltpu.VMEM)),
        scratch_shapes=[pltpu.VMEM((n, n), F32), pltpu.SemaphoreType.DMA],
        compiler_params=pltpu.CompilerParams(vmem_limit_bytes=24 << 20),
        name="plane",
    )(recv, left, right, twiddle, shell)


def local(field, shell):
    fields, cx, cy, nz = field.shape
    n_row = lax.axis_size(ROW)
    n_col = lax.axis_size(COL)
    devices = n_row * n_col
    nx, ny, keep = cx * n_row, cy * n_col, nz // 2
    sizes = tuple(lax.axis_size(axis) for axis in ROW_COL)
    left, right, twiddle = plane_tables(n_row, sizes)
    scale = 1.0 / (float(nx) * ny * nz)
    unit = float(SHELLS) / (keep * ny * nx)
    sent = depth_call(field.reshape(cx * cy, nz), jnp.asarray(depth_tables(nz, sizes)), odd_step(sizes))
    sent = sent.reshape(devices, 4, 128)
    got = lax.all_to_all(sent, PEERS, 0, 0, tiled=True)
    got = got.reshape(devices * 4, 128)
    power, sums = plane_call(got, left, right, twiddle, shell.reshape(ny, nx), scale, unit)
    sums = sums + lax.ppermute(sums, CORE, [(0, 1), (1, 0)])
    chips = devices // lax.axis_size(CORE)
    sums = jnp.broadcast_to(sums, (chips, 2, 128))
    sums = lax.all_to_all(sums, CHIPS, 0, 0, tiled=True)
    spectrum = jnp.sum(sums, axis=0).reshape(fields, SHELLS)
    return (power.reshape(fields, 1, ny, nx), spectrum)


def solution(mesh):
    split = Mesh(mesh.devices.reshape(4, 2, 2, 2, 4, 2), ROW_COL)
    in_specs = (P(None, ROW, COL, None), P(ROW_COL, None, None))
    out_specs = (P(None, ROW_COL, None, None), P())
    return jax.shard_map(local, mesh=split, in_specs=in_specs, out_specs=out_specs, check_vma=False)
```

```python
import functools
import itertools
import math

import jax
import jax.numpy as jnp
import numpy as np
from jax import lax
from jax.experimental import pallas as pl
from jax.experimental.pallas import tpu as pltpu
from jax.sharding import Mesh
from jax.sharding import PartitionSpec as P

SHELLS = 256
ROW = ("row_0", "row_1", "row_2")
COL = ("col_0", "col_1", "col_2")
ROW_COL = ROW + COL
CORE = "row_2"
PEERS = ("row_0", "col_0", "col_1", "col_2", "row_1", "row_2")
CHIPS = ("col_1", "col_2", "col_0", "row_0", "row_1")
F32 = jnp.float32
BF16 = jnp.bfloat16


def split_table(table):
    upper = table.astype(np.float32).astype(BF16)
    lower = (table - upper.astype(np.float64)).astype(np.float32).astype(BF16)
    return np.stack([upper, lower])


def peer_order(sizes):
    ranks = np.arange(math.prod(sizes)).reshape(sizes)
    return ranks.transpose([ROW_COL.index(axis) for axis in PEERS]).reshape(-1)


def odd_step(sizes):
    return math.prod(sizes[ROW_COL.index(axis)] for axis in PEERS[PEERS.index(COL[-1]) + 1 :])


@functools.cache
def depth_tables(nz, sizes):
    order = peer_order(sizes).reshape(-1, 2, odd_step(sizes))
    z = np.arange(nz // 2)
    out = []
    for parity in range(2):
        k = order[:, parity, :].T.reshape(-1)
        angle = 2.0 * math.pi / nz * (k[:, None] * z[None, :] % nz)
        out.append(split_table(np.concatenate([np.cos(angle), -np.sin(angle)])))
    return np.stack(out)


@functools.cache
def plane_tables(radix, sizes):
    n = np.arange(radix)
    base = np.multiply.outer(n, n)
    both = base[:, None, :, None] + base[None, :, None, :]
    both = both.reshape(radix * radix, radix * radix)
    angle = 2.0 * math.pi / radix * (both % radix)
    cos, sin = np.cos(angle), -np.sin(angle)
    square = np.stack([split_table(table) for table in (cos, sin - cos, cos + sin)])
    angle = 2.0 * math.pi / (radix * radix) * both
    twiddle = np.stack([np.cos(angle), -np.sin(angle)]).astype(np.float32)
    return np.ascontiguousarray(square[..., peer_order(sizes)]), square, twiddle


def split_two(values):
    upper = values.astype(BF16)
    return upper, (values - upper.astype(F32)).astype(BF16)


NN = (((1,), (0,)), ((), ()))
NT = (((1,), (1,)), ((), ()))


def dot3(lhs, rhs, dims):
    dot = functools.partial(lax.dot_general, dimension_numbers=dims, preferred_element_type=F32)
    return dot(lhs[0], rhs[0]) + dot(lhs[0], rhs[1]) + dot(lhs[1], rhs[0])


def depth_kernel(step, field_hbm, table_hbm, out_ref, field_ref, table_ref, sems):
    copies = [
        pltpu.make_async_copy(field_hbm, field_ref, sems.at[0]),
        pltpu.make_async_copy(table_hbm, table_ref, sems.at[1]),
    ]
    for copy in copies:
        copy.start()
    for copy in copies:
        copy.wait()
    half = field_ref.shape[1] // 2
    lanes = field_ref.shape[0] // 2
    freqs = table_ref.shape[2] // 2
    near = field_ref[:, :half]
    far = field_ref[:, half:]
    for parity in range(2):
        folded = split_two(near + far if parity == 0 else near - far)
        spec = dot3((table_ref[parity, 0], table_ref[parity, 1]), folded, NT)
        count = freqs // step
        for part, low, side in itertools.product(range(2), range(step), range(2)):
            start = part * freqs + low * count
            block = spec[start : start + count, side * lanes : (side + 1) * lanes]
            start = (parity * step + low) * 4 + part * 2 + side
            out_ref[pl.ds(start, count, stride=8 * step), :] = block


def swap_digits(blocks, radix):
    lane = lax.broadcasted_iota(jnp.int32, blocks[0].shape, 1)
    width = blocks[0].shape[1]
    step = 1
    while step < radix:
        low = (lane & step) == 0
        out = list(blocks)
        for i in range(radix):
            if i & step:
                continue
            a, b = blocks[i], blocks[i + step]
            out[i] = jnp.where(low, a, pltpu.roll(b, step, 1))
            out[i + step] = jnp.where(low, pltpu.roll(a, width - step, 1), b)
        blocks = out
        step *= 2
    return blocks


def plane_kernel(
    scale, unit, recv_ref, left_ref, right_ref, twiddle_ref, shell_ref, power_hbm, sums_ref, power_ref, sem
):
    n = power_ref.shape[0]
    radix = math.isqrt(n)
    parts = [
        jnp.concatenate([recv_ref[pl.ds(2 * c + s, n, stride=4), :] for s in range(2)], axis=1)
        for c in range(2)
    ]
    tables = [(left_ref[i, 0], left_ref[i, 1]) for i in range(3)]
    factors = [split_two(x) for x in (parts[0] + parts[1], parts[0], parts[1])]
    both, more, less = [dot3(t, x, NN) for t, x in zip(tables, factors)]
    u_re, u_im = both - less, both + more
    t_re, t_im = twiddle_ref[0], twiddle_ref[1]
    re = u_re * t_re - u_im * t_im
    im = u_re * t_im + u_im * t_re
    tables = [(right_ref[i, 0], right_ref[i, 1]) for i in range(3)]
    factors = [split_two(x) for x in (re + im, re, im)]
    both, more, less = [dot3(x, t, NN) for t, x in zip(tables, factors)]
    v_re, v_im = both - less, both + more
    power = (v_re * v_re + v_im * v_im) * scale
    half = n // 2
    picks = []
    marked = []
    for side in range(2):
        lanes = slice(side * half, (side + 1) * half)
        blocks = [power[a * radix : (a + 1) * radix, lanes] for a in range(radix)]
        for index, tile in enumerate(swap_digits(blocks, radix)):
            rows = slice(index * radix, (index + 1) * radix)
            power_ref[rows, lanes] = tile
            upper, lower = split_two(tile)
            marks = shell_ref[rows, lanes]
            high = (marks >> 4).astype(F32).astype(BF16)
            low = (marks & 15).astype(F32).astype(BF16)
            zero = jnp.zeros_like(upper)
            one = jnp.ones_like(upper)
            flags = [high == jnp.array(h, BF16) for h in range(16)]
            picked = [jnp.where(flag, piece, zero) for piece in (upper, lower) for flag in flags]
            picks.append(jnp.concatenate(picked, axis=0))
            flags = [low == jnp.array(l, BF16) for l in range(16)]
            picked = [jnp.where(flag, one, zero) for flag in flags]
            marked.append(jnp.concatenate(picked, axis=0))
    copy = pltpu.make_async_copy(power_ref, power_hbm, sem)
    copy.start()
    dot = functools.partial(lax.dot_general, preferred_element_type=F32)
    acc = dot(jnp.concatenate(picks, axis=1), jnp.concatenate(marked, axis=1), NT)
    acc = acc[:SHELLS, :] + acc[SHELLS:, :]
    row = lax.broadcasted_iota(jnp.int32, (256, 256), 0)
    lane = lax.broadcasted_iota(jnp.int32, (256, 256), 1)
    same = jnp.where((row & 15) == (lane & 15), acc, 0.0).reshape(16, 16, 256)
    by_high = (same[:, :8, :] + same[:, 8:, :]).reshape(128, 256)
    spread = ((row >> 4) == (lane & 15)).astype(F32).astype(BF16)
    upper, lower = split_two(by_high)
    wide = dot(upper, spread, NN) + dot(lower, spread, NN)
    row = lax.broadcasted_iota(jnp.int32, (128, 256), 0)
    lane = lax.broadcasted_iota(jnp.int32, (128, 256), 1)
    sums = jnp.sum(jnp.where((lane >> 4) == (row >> 3), wide, 0.0), axis=0, keepdims=True) * unit
    for side in range(2):
        sums_ref[side : side + 1, :] = sums[:, side * 128 : (side + 1) * 128]
    copy.wait()


def depth_call(field, tables, step):
    rows = field.shape[0]
    field = pltpu.with_memory_space_constraint(field, pltpu.HBM)
    tables = pltpu.with_memory_space_constraint(tables, pltpu.HBM)
    return pl.pallas_call(
        functools.partial(depth_kernel, step),
        in_specs=[pl.BlockSpec(memory_space=pltpu.HBM)] * 2,
        out_shape=jax.ShapeDtypeStruct((field.shape[1] // 2 * 4, rows // 2), F32),
        scratch_shapes=[
            pltpu.VMEM(field.shape, field.dtype),
            pltpu.VMEM(tables.shape, tables.dtype),
            pltpu.SemaphoreType.DMA((2,)),
        ],
        compiler_params=pltpu.CompilerParams(vmem_limit_bytes=12 << 20),
        name="depth",
    )(field, tables)


def plane_call(recv, left, right, twiddle, shell, scale, unit):
    n = shell.shape[0]
    return pl.pallas_call(
        functools.partial(plane_kernel, scale, unit),
        out_shape=(
            jax.ShapeDtypeStruct((n, n), F32),
            jax.ShapeDtypeStruct((2, 128), F32),
        ),
        out_specs=(pl.BlockSpec(memory_space=pltpu.HBM), pl.BlockSpec(memory_space=pltpu.VMEM)),
        scratch_shapes=[pltpu.VMEM((n, n), F32), pltpu.SemaphoreType.DMA],
        compiler_params=pltpu.CompilerParams(vmem_limit_bytes=24 << 20),
        name="plane",
    )(recv, left, right, twiddle, shell)


def local(field, shell):
    fields, cx, cy, nz = field.shape
    n_row = lax.axis_size(ROW)
    n_col = lax.axis_size(COL)
    devices = n_row * n_col
    nx, ny, keep = cx * n_row, cy * n_col, nz // 2
    sizes = tuple(lax.axis_size(axis) for axis in ROW_COL)
    left, right, twiddle = plane_tables(n_row, sizes)
    scale = 1.0 / (float(nx) * ny * nz)
    unit = float(SHELLS) / (keep * ny * nx)
    sent = depth_call(field.reshape(cx * cy, nz), jnp.asarray(depth_tables(nz, sizes)), odd_step(sizes))
    sent = sent.reshape(devices, 4, 128)
    got = lax.all_to_all(sent, PEERS, 0, 0, tiled=True)
    got = got.reshape(devices * 4, 128)
    power, sums = plane_call(got, left, right, twiddle, shell.reshape(ny, nx), scale, unit)
    sums = sums + lax.ppermute(sums, CORE, [(0, 1), (1, 0)])
    chips = devices // lax.axis_size(CORE)
    sums = jnp.broadcast_to(sums, (chips, 2, 128))
    sums = lax.all_to_all(sums, CHIPS, 0, 0, tiled=True)
    spectrum = jnp.sum(sums, axis=0).reshape(fields, SHELLS)
    return (power.reshape(fields, 1, ny, nx), spectrum)


def solution(mesh):
    split = Mesh(mesh.devices.reshape(4, 2, 2, 2, 4, 2), ROW_COL)
    in_specs = (P(None, ROW, COL, None), P(ROW_COL, None, None))
    out_specs = (P(None, ROW_COL, None, None), P())
    return jax.shard_map(local, mesh=split, in_specs=in_specs, out_specs=out_specs, check_vma=False)
```
